512 devices in a mesh: groups: 2 (over y), expert: 32 (over z, core), mp: 8 (over x).
Axes of the slice: x: 8, y: 2, z: 16, core: 2. Of those that a mesh axis runs over, the one named last changes fastest.
The devices are a block of a 8x16x16 slice.
Arguments:
- tokens: bfloat16 [49152, 1024], P(('groups', 'expert'), 'mp'), parts along dimension 0, may hold values from -60 to 60
- gain: float32 [1024], replicated, may hold values from 0.1 to 1.9
- w_res_in: bfloat16 [1024, 4096], P(None, 'mp'), may hold values from -0.1875 to 0.1875
- w_res_out: bfloat16 [4096, 1024], P('mp'), may hold values from -0.09375 to 0.09375
- w_exp_in: bfloat16 [32, 1024, 4096], P('expert', None, 'mp'), may hold values from -0.1875 to 0.1875
- w_exp_out: bfloat16 [32, 4096, 1024], P('expert', 'mp'), may hold values from -0.09375 to 0.09375
- expert_of: int32 [49152], P(('groups', 'expert')), parts along dimension 0, may hold values from 0 to 31
- slot_of: int32 [49152], P(('groups', 'expert')), parts along dimension 0, may hold values from -1 to 29, as said below
- gate_prob: float32 [49152], P(('groups', 'expert')), parts along dimension 0, may hold values from 0.2 to 1
Outputs:
- layer_out: bfloat16 [49152, 1024], P(('groups', 'expert'), 'mp'), parts along dimension 0
The draws below stay inside these ranges and needn't reach their ends.
There are 2 independent parts, one for each index of `groups`. The reference program is written for one: setup_inputs(seed, part) draws one part's arguments, and reference() takes and returns one part's arrays. A program takes and returns all parts, laid end to end along the dimension named above; an argument that names none is the same for every part. Nothing has to cross between parts.
Inputs may be any that keep to these rules, and one draw needn't show every extreme that they name: slot_of[t] is the number of earlier tokens of t's aligned block of 768 tokens with the same expert_of, or -1 where that number is 30 or more. In every draw one expert has more than 30 tokens in every aligned block.
All inputs are finite; a program needn't handle non-finite values.
Results may differ from the reference program's by a relative error of at most 0.014.
Values may be sent and summed in bfloat16 or wider, within the bound.
A program may use at most 64 MiB of HBM per device.

```python
import math
import jax
import jax.numpy as jnp
from jax import lax

D = 1024
FE = 4096
FR = 4096
TOK_DEV = 768
EXPERTS = 32
TOKENS = 24576
CAP = 30
N_EXPERT = 32
N_MP = 8


def draw_tokens(key, part):
    mixed = jax.random.fold_in(key, 11)
    key_base, key_rows, key_cols = jax.random.split(mixed, 3)
    base = jnp.clip(jax.random.normal(key_base, (TOKENS, D), jnp.float32), -5.5, 5.5)
    row_scale = jnp.exp(jax.random.uniform(key_rows, (TOKENS, 1), jnp.float32) * math.log(10.0))
    col_scale = jnp.exp(jax.random.uniform(key_cols, (1, D), jnp.float32) * math.log(10.0))
    return (base * row_scale * col_scale / 10.0).astype(jnp.bfloat16)


def shuffle(subkey):
    return jax.random.permutation(subkey, TOK_DEV)


def routing_pair(key):
    mixed = jax.random.fold_in(key, 5)
    key_base, key_hot, key_perm = jax.random.split(mixed, 3)
    blocks = TOKENS // TOK_DEV
    base = jax.random.randint(key_base, (blocks, TOK_DEV), 0, EXPERTS)
    hottest = jax.random.randint(key_hot, (1, 1), 0, EXPERTS)
    order = jax.vmap(shuffle)(jax.random.split(key_perm, blocks))
    chosen = order < CAP + 2
    expert_ids = jnp.where(chosen, hottest, base).astype(jnp.int32)
    same = expert_ids[:, :, None] == expert_ids[:, None, :]
    index = jnp.arange(TOK_DEV, dtype=jnp.int32)
    earlier = index[None, :] < index[:, None]
    rank = jnp.sum(jnp.logical_and(same, earlier[None]).astype(jnp.int32), axis=2)
    slots = jnp.where(rank < CAP, rank, -1).astype(jnp.int32)
    return (expert_ids.reshape(TOKENS), slots.reshape(TOKENS))


def draw_expert_of(key, part):
    return routing_pair(key)[0]


def draw_slot_of(key, part):
    return routing_pair(key)[1]


def level_of(own_key, extent, shards, low, largest):
    loudness = 1.0
    for axis_at, parts in shards:
        heights = jax.random.uniform(jax.random.fold_in(jax.random.fold_in(own_key, 6), axis_at), (parts,), jnp.float32, low / len(shards), largest / len(shards))
        loudness = loudness * jnp.repeat(jnp.exp(heights), extent[axis_at] // parts).reshape((-1,) + (1,) * (len(extent) - 1 - axis_at))
    return loudness


def gaussian(stream_key, dims, deviation, most, shards=(), kind=jnp.bfloat16):
    result = jax.random.normal(stream_key, dims, jnp.float32) * deviation
    if len(shards) > 0:
        result = level_of(stream_key, dims, shards, -0.22, 0.18) * result
    return jnp.clip(result, min=-most, max=most).astype(kind)


def setup_inputs(seed: int = 0, part: int = 0) -> dict:
    arg_keys = jax.random.split(jax.random.key(seed), 10)
    part_keys = jax.random.split(jax.random.fold_in(arg_keys[9], part), 10)
    return {
        "tokens": draw_tokens(jax.random.fold_in(jax.random.fold_in(arg_keys[9], part), 71), part),
        "gain": jnp.clip(1.0 + 0.18 * jax.random.normal(arg_keys[1], (D,), jnp.float32), 0.1, 1.9),
        "w_res_in": gaussian(arg_keys[2], (D, FR), D ** -0.5, 0.1875, ((1, 8),)),
        "w_res_out": gaussian(arg_keys[3], (FR, D), FR ** -0.5, 0.09375, ((0, 8),)),
        "w_exp_in": gaussian(arg_keys[4], (EXPERTS, D, FE), D ** -0.5, 0.1875, ((0, 32), (2, 8))),
        "w_exp_out": gaussian(arg_keys[5], (EXPERTS, FE, D), FE ** -0.5, 0.09375, ((0, 32), (1, 8))),
        "expert_of": draw_expert_of(jax.random.fold_in(jax.random.fold_in(arg_keys[9], part), 71), part),
        "slot_of": draw_slot_of(jax.random.fold_in(jax.random.fold_in(arg_keys[9], part), 71), part),
        "gate_prob": jnp.clip(jnp.exp(math.log(1.0) - 1.609438 * jax.random.uniform(part_keys[8], (TOKENS,), jnp.float32) ** level_of(part_keys[8], (TOKENS,), ((0, 32),), -0.2, 0.2)), 0.2, 1.0),
    }


def rms_rows(tokens, gain):
    values = tokens.astype(jnp.float32)
    inverse = lax.rsqrt(lax.optimization_barrier(jnp.mean(values * values, axis=-1, keepdims=True)) + 1e-05)
    return (values * inverse * gain.astype(jnp.float32)).astype(jnp.bfloat16)

def block_sums(hidden, w_out):
    width = hidden.shape[1] // N_MP
    total = jnp.zeros((hidden.shape[0], w_out.shape[1]), jnp.float32)
    for block in range(N_MP):
        part = jnp.dot(hidden[:, block * width:(block + 1) * width], w_out[block * width:(block + 1) * width], preferred_element_type=jnp.float32)
        total = total + part.astype(jnp.bfloat16).astype(jnp.float32)
    return total

def reference(tokens, gain, w_res_in, w_res_out, w_exp_in, w_exp_out, expert_of, slot_of, gate_prob):
    normed = rms_rows(tokens, gain)
    res_hidden = jax.nn.gelu(jnp.dot(normed, w_res_in, preferred_element_type=jnp.float32)).astype(jnp.bfloat16)
    res_sum = block_sums(res_hidden, w_res_out)
    blocks = N_EXPERT
    position = jnp.arange(TOKENS, dtype=jnp.int32)
    block_of = position // TOK_DEV
    slots_all = EXPERTS * blocks * CAP
    destination = jnp.where(slot_of >= 0, expert_of * (blocks * CAP) + block_of * CAP + slot_of, slots_all).astype(jnp.int32)
    buffer = jnp.zeros((slots_all + 1, D), jnp.bfloat16).at[destination].set(normed)
    expert_in = buffer[:slots_all].reshape(EXPERTS, blocks * CAP, D)

    def one_expert(item):
        rows, w_in, w_out = item
        hidden = jax.nn.gelu(jnp.dot(rows, w_in, preferred_element_type=jnp.float32)).astype(jnp.bfloat16)
        return block_sums(hidden, w_out).astype(jnp.bfloat16)
    expert_out = lax.map(one_expert, (expert_in, w_exp_in, w_exp_out))
    flat_rows = jnp.concatenate([expert_out.reshape(slots_all, D), jnp.zeros((1, D), jnp.bfloat16)], axis=0)
    moe_value = flat_rows[destination].astype(jnp.float32)
    return (res_sum + gate_prob[:, None] * moe_value).astype(jnp.bfloat16)
```

```python
import functools

import jax
import jax.numpy as jnp
from jax import lax
from jax.experimental import pallas as pl
from jax.experimental.pallas import tpu as pltpu
from jax.sharding import PartitionSpec as P

MESH = pl.DeviceIdType.MESH
BF16 = jnp.bfloat16
F32 = jnp.float32


def rms_rows(pieces, gain):
    values = jnp.concatenate([piece.astype(F32) for piece in pieces], axis=1)
    inverse = lax.rsqrt(jnp.mean(values * values, axis=-1, keepdims=True) + 1e-05)
    return (values * inverse * gain).astype(BF16)


def mlp_rows(rows, w_in, w_out):
    hidden = jax.nn.gelu(jnp.dot(rows, w_in[...], preferred_element_type=F32)).astype(BF16)
    return jnp.dot(hidden, w_out[...], preferred_element_type=F32)


def remote(src, dst, send_sem, recv_sem, axis, device):
    return pltpu.make_async_remote_copy(
        src_ref=src,
        dst_ref=dst,
        send_sem=send_sem,
        recv_sem=recv_sem,
        device_id={axis: device},
        device_id_type=MESH,
    )


def layer_kernel(
    experts, ring, slots, chunks,
    meta, tok_hbm, wri_hbm, wro_hbm, wei_hbm, weo_hbm, out,
    tok_all, exp_all, outgoing, wri, wro, wei, weo, res_part, exp_part,
    rs_send, rs_recv, es_send, es_recv, ret_send, returned, table, gate_cols,
    local_sem, tok_ss, tok_rs, exp_ss, exp_rs, dis_ss, dis_rs,
    rs_ss, rs_rs, es_ss, es_rs, ret_ss, ret_rs,
):
    me = lax.axis_index("mp")
    mine = lax.axis_index("expert")
    tokens, width = out.shape
    total = experts * slots
    messages = ring - 1
    chunk_rows = total // chunks

    def on_ring(offset):
        return lax.rem(me + offset + 2 * ring, ring)

    def partner(p):
        far = lax.div(p + 1, 2)
        return experts // 2 + jnp.where(lax.rem(p, 2) == 0, far, -far)

    barrier = pltpu.get_barrier_semaphore()
    for offset in (-1, 1):
        pl.semaphore_signal(
            barrier, inc=1, device_id={"mp": on_ring(offset)}, device_id_type=MESH
        )

    def greet(step, carry):
        pl.semaphore_signal(
            barrier,
            inc=1,
            device_id={"expert": lax.rem(mine + step, experts)},
            device_id_type=MESH,
        )
        return carry

    lax.fori_loop(1, experts, greet, 0)

    tok_copy = pltpu.make_async_copy(tok_hbm, tok_all.at[me], local_sem.at[0])
    tok_copy.start()
    weight_copies = [
        pltpu.make_async_copy(src, dst, local_sem.at[1 + at])
        for at, (src, dst) in enumerate(
            ((wri_hbm, wri), (wro_hbm, wro), (wei_hbm, wei), (weo_hbm, weo))
        )
    ]
    for copy in weight_copies:
        copy.start()
    tok_copy.wait()

    slot_row = meta[0:1, 0:tokens]

    def pick(step, carry):
        rows = pl.ds(pl.multiple_of(step * chunk_rows, chunk_rows), chunk_rows)
        index = lax.broadcasted_iota(jnp.int32, (chunk_rows, tokens), 0) + step * chunk_rows
        one_hot = jnp.where(index.astype(F32) == slot_row, 1.0, 0.0).astype(BF16)
        outgoing[rows, :] = jnp.dot(
            one_hot, tok_all[me], preferred_element_type=F32
        ).astype(BF16)
        return carry

    lax.fori_loop(0, chunks, pick, 0)
    pl.semaphore_wait(barrier, experts + 1)

    def gather_copy(buf, send_sem, recv_sem, j, way, arriving):
        turn = 1 - 2 * way
        half = buf.shape[1] // 2
        shard = on_ring(-turn * (j // 2 + (1 if arriving else 0)))
        ref = buf.at[shard, pl.ds(((j + way) % 2) * half, half)]
        return remote(ref, ref, send_sem.at[way, j], recv_sem.at[way, j], "mp", on_ring(turn))

    def gather_send(ring_refs, j):
        for way in (0, 1):
            gather_copy(*ring_refs, j, way, False).start()

    def gather_step(ring_refs, j):
        for way in (0, 1):
            gather_copy(*ring_refs, j, way, True).wait_recv()
            if j + 2 < messages:
                gather_copy(*ring_refs, j + 2, way, False).start()

    tok_ring = (tok_all, tok_ss, tok_rs)
    exp_ring = (exp_all, exp_ss, exp_rs)
    gather_send(tok_ring, 0)

    def block(at):
        return pl.ds(pl.multiple_of(at * slots, slots), slots)

    def dispatch(p, carry):
        target = lax.rem(mine - partner(p) + experts, experts)
        remote(
            outgoing.at[block(target)], exp_all.at[me, block(p)],
            dis_ss.at[0], dis_rs.at[0], "expert", target,
        ).start()
        return carry

    lax.fori_loop(0, experts - 1, dispatch, 0)
    own_copy = pltpu.make_async_copy(
        outgoing.at[block(mine)], exp_all.at[me, block(experts - 1)], local_sem.at[5]
    )
    own_copy.start()
    gather_send(tok_ring, 1)

    def turned(row):
        return jnp.transpose(jnp.broadcast_to(row, (width, tokens)))

    gate_cols[...] = turned(meta[1:2, 0:tokens])
    slot_cols = turned(slot_row)
    lane = lax.broadcasted_iota(jnp.int32, (tokens, width), 1)
    for at in range(0, total, width):
        wide = min(width, total - at)
        hit = jnp.where((lane + at).astype(F32) == slot_cols, 1.0, 0.0).astype(BF16)
        table[:, at : at + wide] = hit[:, :wide]

    for j in range(messages - 2):
        gather_step(tok_ring, j)

    others = pl.ds(0, (experts - 1) * slots)

    def all_dispatched():
        return remote(
            outgoing.at[others], exp_all.at[me, others], dis_ss.at[0], dis_rs.at[0], "expert",
            lax.rem(mine + 1, experts),
        )

    own_copy.wait()
    all_dispatched().wait_recv()
    gather_send(exp_ring, 0)
    gather_send(exp_ring, 1)
    for j in range(messages - 2, messages):
        gather_step(tok_ring, j)

    gain = meta[2:3, 0 : ring * width]
    weight_copies[0].wait()
    weight_copies[1].wait()
    res_rows = tokens // 3 if tokens % 48 == 0 else tokens

    def residual(step, carry):
        rows = pl.ds(pl.multiple_of(step * res_rows, res_rows), res_rows)
        normed = rms_rows([tok_all[k, rows, :] for k in range(ring)], gain)
        part = mlp_rows(normed, wri, wro)
        for k in range(ring):
            res_part[k, rows, :] = part[:, k * width : (k + 1) * width]
        return carry

    lax.fori_loop(0, tokens // res_rows, residual, 0)

    def scatter_copy(refs, c, j, way):
        send, recv, send_sem, recv_sem = refs[1:]
        return remote(
            send.at[way, c, j], recv.at[way, c, j],
            send_sem.at[way, c, j], recv_sem.at[way, c, j], "mp", on_ring(1 - 2 * way),
        )

    def scatter_send(refs, c, j):
        part, send, recv = refs[:3]
        half = send.shape[3]
        for way in (0, 1):
            turn = 1 - 2 * way
            dest = on_ring(turn * (ring // 2 - (j + 1) // 2))
            start = pl.multiple_of(c * 2 * half + ((j + way) % 2) * half, half)
            value = part[dest, pl.ds(start, half), :]
            if j >= 2:
                scatter_copy(refs, c, j - 2, way).wait_recv()
                value = value + recv[way, c, j - 2].astype(F32)
            send[way, c, j] = value.astype(BF16)
            scatter_copy(refs, c, j, way).start()

    def scatter_sum(refs, c, h):
        part, send, recv = refs[:3]
        half = send.shape[3]
        start = pl.multiple_of(c * 2 * half + h * half, half)
        value = part[me, pl.ds(start, half), :]
        for way in (0, 1):
            j = messages - 1 if h == way else messages - 2
            scatter_copy(refs, c, j, way).wait_recv()
            value = value + recv[way, c, j].astype(F32)
        return value

    res_sums = (res_part, rs_send, rs_recv, rs_ss, rs_rs)
    exp_sums = (exp_part, es_send, es_recv, es_ss, es_rs)

    for j in range(messages - 2):
        gather_step(exp_ring, j)
    scatter_send(res_sums, 0, 0)
    scatter_send(res_sums, 0, 1)
    for j in range(messages - 2, messages):
        gather_step(exp_ring, j)

    weight_copies[2].wait()
    weight_copies[3].wait()

    def expert(c, carry):
        rows = pl.ds(pl.multiple_of(c * chunk_rows, chunk_rows), chunk_rows)
        normed = rms_rows([exp_all[k, rows, :] for k in range(ring)], gain)
        part = mlp_rows(normed, wei, weo)
        for k in range(ring):
            exp_part[k, rows, :] = part[:, k * width : (k + 1) * width]
        scatter_send(exp_sums, c, 0)
        scatter_send(exp_sums, c, 1)
        return carry

    lax.fori_loop(0, chunks, expert, 0)

    for j in range(2, messages):

        def wave(c, carry, j=j):
            scatter_send(exp_sums, c, j)
            return carry

        lax.fori_loop(0, chunks, wave, 0)

    early = min(4, messages)
    for j in range(2, early):
        scatter_send(res_sums, 0, j)

    def give_back(p, carry):
        source = lax.rem(mine + partner(p), experts)
        remote(
            ret_send.at[block(p)], returned.at[block(mine)],
            ret_ss.at[0], ret_rs.at[0], "expert", source,
        ).start()
        return carry

    per_chunk = experts // chunks
    half_rows = chunk_rows // 2
    for c in range(chunks):
        for h in (0, 1):
            ret_send[pl.ds(c * chunk_rows + h * half_rows, half_rows), :] = scatter_sum(
                exp_sums, c, h
            ).astype(BF16)
        last = experts - 1 if c == chunks - 1 else (c + 1) * per_chunk
        lax.fori_loop(c * per_chunk, last, give_back, 0)
    own_back = pltpu.make_async_copy(
        ret_send.at[block(experts - 1)], returned.at[block(mine)], local_sem.at[5]
    )
    own_back.start()

    for j in range(early, messages):
        scatter_send(res_sums, 0, j)
    half = tokens // 2
    sums = [scatter_sum(res_sums, 0, h) for h in (0, 1)]

    own_back.wait()

    def all_returned():
        return remote(
            ret_send.at[others], returned.at[others], ret_ss.at[0], ret_rs.at[0], "expert",
            lax.rem(mine + 1, experts),
        )

    all_returned().wait_recv()
    for h in (0, 1):
        rows = pl.ds(h * half, half)
        moe = jnp.dot(table[rows, :], returned[...], preferred_element_type=F32)
        out[rows, :] = (sums[h] + gate_cols[rows, :] * moe).astype(BF16)

    all_dispatched().wait_send()
    all_returned().wait_send()
    for j in range(messages):
        for way in (0, 1):
            gather_copy(*tok_ring, j, way, False).wait_send()
            gather_copy(*exp_ring, j, way, False).wait_send()
            scatter_copy(res_sums, 0, j, way).wait_send()

    def drain(c, carry):
        for j in range(messages):
            for way in (0, 1):
                scatter_copy(exp_sums, c, j, way).wait_send()
        return carry

    lax.fori_loop(0, chunks, drain, 0)


def per_device(
    experts, ring, tokens, gain, w_res_in, w_res_out, w_exp_in, w_exp_out,
    expert_of, slot_of, gate_prob,
):
    count, width = tokens.shape
    model, hidden = w_res_in.shape
    capacity = max(2, 5 * count // (4 * experts))
    slots = -(-capacity // 16) * 16
    chunks = 4
    total = experts * slots
    messages = ring - 1

    slot_id = jnp.where(slot_of >= 0, expert_of * slots + slot_of, -1).astype(F32)
    span = max(count, model)
    meta = jnp.stack(
        [
            jnp.pad(slot_id, (0, span - count)),
            jnp.pad(gate_prob, (0, span - count)),
            jnp.pad(gain, (0, span - model)),
        ]
    )
    any_space = pl.BlockSpec(memory_space=pl.ANY)
    in_vmem = pl.BlockSpec(memory_space=pltpu.VMEM)
    sems = pltpu.SemaphoreType.DMA
    res_half, exp_half = count // 2, total // chunks // 2
    return pl.pallas_call(
        functools.partial(layer_kernel, experts, ring, slots, chunks),
        out_shape=jax.ShapeDtypeStruct((count, width), BF16),
        in_specs=[in_vmem] + [any_space] * 5,
        out_specs=in_vmem,
        scratch_shapes=[
            pltpu.VMEM((ring, count, width), BF16),
            pltpu.VMEM((ring, total, width), BF16),
            pltpu.VMEM((total, width), BF16),
            pltpu.VMEM((model, hidden), BF16),
            pltpu.VMEM((hidden, model), BF16),
            pltpu.VMEM((model, hidden), BF16),
            pltpu.VMEM((hidden, model), BF16),
            pltpu.VMEM((ring, count, width), F32),
            pltpu.VMEM((ring, total, width), F32),
            pltpu.VMEM((2, 1, messages, res_half, width), BF16),
            pltpu.VMEM((2, 1, messages, res_half, width), BF16),
            pltpu.VMEM((2, chunks, messages, exp_half, width), BF16),
            pltpu.VMEM((2, chunks, messages, exp_half, width), BF16),
            pltpu.VMEM((total, width), BF16),
            pltpu.VMEM((total, width), BF16),
            pltpu.VMEM((count, total), BF16),
            pltpu.VMEM((count, width), F32),
            sems((6,)),
            sems((2, messages)),
            sems((2, messages)),
            sems((2, messages)),
            sems((2, messages)),
            sems((1,)),
            sems((1,)),
            sems((2, 1, messages)),
            sems((2, 1, messages)),
            sems((2, chunks, messages)),
            sems((2, chunks, messages)),
            sems((1,)),
            sems((1,)),
        ],
        compiler_params=pltpu.CompilerParams(
            collective_id=0, has_side_effects=True, vmem_limit_bytes=56 * 1024 * 1024
        ),
        name="moe_layer",
    )(meta, tokens, w_res_in, w_res_out, w_exp_in[0], w_exp_out[0])


def solution(mesh):
    return jax.shard_map(
        functools.partial(per_device, mesh.shape["expert"], mesh.shape["mp"]),
        mesh=mesh,
        in_specs=(
            P(("groups", "expert"), "mp"),
            P(),
            P(None, "mp"),
            P("mp", None),
            P("expert", None, "mp"),
            P("expert", "mp", None),
            P(("groups", "expert")),
            P(("groups", "expert")),
            P(("groups", "expert")),
        ),
        out_specs=P(("groups", "expert"), "mp"),
        check_vma=False,
    )
```

```python
import functools

import jax
import jax.numpy as jnp
from jax import lax
from jax.experimental import pallas as pl
from jax.experimental.pallas import tpu as pltpu
from jax.sharding import PartitionSpec as P

MESH = pl.DeviceIdType.MESH
BF16 = jnp.bfloat16
F32 = jnp.float32


def rms_rows(pieces, gain):
    values = jnp.concatenate([piece.astype(F32) for piece in pieces], axis=1)
    inverse = lax.rsqrt(jnp.mean(values * values, axis=-1, keepdims=True) + 1e-05)
    return (values * inverse * gain).astype(BF16)


def mlp_rows(rows, w_in, w_out):
    hidden = jax.nn.gelu(jnp.dot(rows, w_in[...], preferred_element_type=F32)).astype(BF16)
    return jnp.dot(hidden, w_out[...], preferred_element_type=F32)


def remote(src, dst, send_sem, recv_sem, axis, device):
    return pltpu.make_async_remote_copy(
        src_ref=src,
        dst_ref=dst,
        send_sem=send_sem,
        recv_sem=recv_sem,
        device_id={axis: device},
        device_id_type=MESH,
    )


def layer_kernel(
    experts, ring, slots, chunks,
    ids_hbm, slots_hbm, gate_hbm, gain_hbm, tok_hbm, wri_hbm, wro_hbm, wei_hbm, weo_hbm, out,
    ids, slot, gate, gain_row, tok_all, exp_all, outgoing, near_out, wri, wro, wei, weo,
    res_part, exp_part, rs_send, rs_recv, es_send, es_recv, ret_send, returned,
    near_ret, near_in, table, gate_cols,
    local_sem, tok_ss, tok_rs, exp_ss, exp_rs, dis_ss, dis_rs,
    rs_ss, rs_rs, es_ss, es_rs, ret_ss, ret_rs,
):
    me = lax.axis_index("mp")
    mine = lax.axis_index("expert")
    tokens, width = out.shape
    total = experts * slots
    messages = ring - 1
    chunk_rows = total // chunks
    per_chunk = experts // chunks
    far_blocks = experts - per_chunk
    far_rows = total - chunk_rows

    def on_ring(offset):
        return lax.rem(me + offset + 2 * ring, ring)

    def partner(p):
        far = lax.div(p + 1, 2)
        return experts // 2 + jnp.where(lax.rem(p, 2) == 0, far, -far)

    def expert_at(p):
        return lax.rem(mine - partner(p) + experts, experts)

    def source_at(p):
        return lax.rem(mine + partner(p), experts)

    def block(at):
        return pl.ds(pl.multiple_of(at * slots, slots), slots)

    def blocks(first, count):
        return pl.ds(first * slots, count * slots)

    barrier = pltpu.get_barrier_semaphore()
    for offset in (-1, 1):
        pl.semaphore_signal(
            barrier, inc=1, device_id={"mp": on_ring(offset)}, device_id_type=MESH
        )

    def greet(step, carry):
        pl.semaphore_signal(
            barrier,
            inc=1,
            device_id={"expert": lax.rem(mine + step, experts)},
            device_id_type=MESH,
        )
        return carry

    lax.fori_loop(1, experts, greet, 0)

    tok_copy = pltpu.make_async_copy(tok_hbm, tok_all.at[me], local_sem.at[0])
    tok_copy.start()
    small_copies = [
        pltpu.make_async_copy(src, dst, local_sem.at[7 + at])
        for at, (src, dst) in enumerate(
            ((ids_hbm, ids), (slots_hbm, slot), (gate_hbm, gate), (gain_hbm, gain_row))
        )
    ]
    for copy in small_copies:
        copy.start()
    weight_copies = [
        pltpu.make_async_copy(src, dst, local_sem.at[1 + at])
        for at, (src, dst) in enumerate(
            ((wri_hbm, wri), (wro_hbm, wro), (wei_hbm, wei), (weo_hbm, weo))
        )
    ]
    for copy in weight_copies:
        copy.start()
    for copy in small_copies:
        copy.wait()
    tok_copy.wait()
    pl.semaphore_wait(barrier, experts + 1)

    def gather_copy(refs, j, way, arriving):
        buf, rows, send_sem, recv_sem = refs
        turn = 1 - 2 * way
        half = rows // 2
        shard = on_ring(-turn * (j // 2 + (1 if arriving else 0)))
        ref = buf.at[shard, pl.ds(((j + way) % 2) * half, half)]
        return remote(ref, ref, send_sem.at[way, j], recv_sem.at[way, j], "mp", on_ring(turn))

    def gather_send(refs, j):
        for way in (0, 1):
            gather_copy(refs, j, way, False).start()

    def gather_step(refs, j):
        for way in (0, 1):
            gather_copy(refs, j, way, True).wait_recv()
            if j + 2 < messages:
                gather_copy(refs, j + 2, way, False).start()

    tok_ring = (tok_all, tokens, tok_ss, tok_rs)
    exp_ring = (exp_all, far_rows, exp_ss, exp_rs)
    gather_send(tok_ring, 0)
    gather_send(tok_ring, 1)

    def as_row(values):
        return jnp.concatenate([values[at : at + 1] for at in range(values.shape[0])], axis=1)

    slot_row = as_row(jnp.where(slot[...] >= 0, ids[...] * slots + slot[...], -1))

    def send_hits(c):
        step = lax.broadcasted_iota(jnp.int32, (slots, tokens), 0)
        hits = [
            jnp.where(step + expert_at(c * per_chunk + at) * slots == slot_row, 1.0, 0.0)
            for at in range(per_chunk)
        ]
        return jnp.concatenate(hits, axis=0).astype(BF16)

    def dispatch(p, carry):
        remote(
            outgoing.at[block(p)], exp_all.at[me, block(p)],
            dis_ss.at[0], dis_rs.at[0], "expert", expert_at(p),
        ).start()
        return carry

    def pick(c, carry):
        rows = pl.ds(pl.multiple_of(c * chunk_rows, chunk_rows), chunk_rows)
        outgoing[rows, :] = jnp.dot(
            send_hits(c), tok_all[me], preferred_element_type=F32
        ).astype(BF16)
        return lax.fori_loop(c * per_chunk, (c + 1) * per_chunk, dispatch, carry)

    lax.fori_loop(0, chunks - 1, pick, 0)

    def turned(row):
        return jnp.transpose(jnp.broadcast_to(row, (width, tokens)))

    gate_cols[...] = turned(as_row(gate[...]))
    slot_cols = turned(slot_row.astype(F32))
    lane = lax.broadcasted_iota(jnp.int32, (1, total), 1)
    wanted = jnp.zeros((1, total), jnp.int32)
    for p in range(experts):
        inside = jnp.logical_and(lane >= p * slots, lane < (p + 1) * slots)
        wanted = jnp.where(inside, lane + (expert_at(p) - p) * slots, wanted)
    wanted = wanted.astype(F32)
    for at in range(0, total, width):
        wide = min(width, total - at)
        hit = jnp.where(slot_cols[:, :wide] == wanted[:, at : at + wide], 1.0, 0.0)
        table[:, at : at + wide] = hit.astype(BF16)

    for j in range(messages - 2):
        gather_step(tok_ring, j)

    far = blocks(0, far_blocks)

    def all_dispatched():
        return remote(
            outgoing.at[far], exp_all.at[me, far], dis_ss.at[0], dis_rs.at[0], "expert",
            lax.rem(mine + 1, experts),
        )

    all_dispatched().wait_recv()
    gather_send(exp_ring, 0)
    gather_send(exp_ring, 1)
    for j in range(messages - 2, messages):
        gather_step(tok_ring, j)

    near_hits = send_hits(chunks - 1)
    for k in range(ring):
        near_out[k] = jnp.dot(near_hits, tok_all[k], preferred_element_type=F32).astype(BF16)

    def dispatch_near(p, carry):
        remote(
            near_out.at[:, block(p - far_blocks), :], exp_all.at[:, block(p), :],
            dis_ss.at[1], dis_rs.at[1], "expert", expert_at(p),
        ).start()
        return carry

    lax.fori_loop(far_blocks, experts - 1, dispatch_near, 0)
    own_copy = pltpu.make_async_copy(
        near_out.at[:, blocks(per_chunk - 1, 1), :],
        exp_all.at[:, blocks(experts - 1, 1), :],
        local_sem.at[5],
    )
    own_copy.start()

    def all_near():
        return remote(
            near_out.at[:, blocks(0, per_chunk - 1), :],
            exp_all.at[:, blocks(far_blocks, per_chunk - 1), :],
            dis_ss.at[1], dis_rs.at[1], "expert", lax.rem(mine + 1, experts),
        )

    gain = gain_row[...]
    weight_copies[0].wait()
    weight_copies[1].wait()
    tiles = 3 if tokens % 48 == 0 else 1
    res_rows = tokens // tiles
    for tile in range(tiles):
        rows = pl.ds(tile * res_rows, res_rows)
        normed = rms_rows([tok_all[k, rows, :] for k in range(ring)], gain)
        part = mlp_rows(normed, wri, wro)
        for k in range(ring):
            res_part[k, rows, :] = part[:, k * width : (k + 1) * width]
        if tile < messages - 3:
            gather_step(exp_ring, tile)
    done = min(tiles, messages - 3)

    def expert_rows(c):
        rows = pl.ds(pl.multiple_of(c * chunk_rows, chunk_rows), chunk_rows)
        normed = rms_rows([exp_all[k, rows, :] for k in range(ring)], gain)
        return rows, mlp_rows(normed, wei, weo)

    weight_copies[2].wait()
    weight_copies[3].wait()
    own_copy.wait()
    all_near().wait_recv()
    near_ret[...] = expert_rows(chunks - 1)[1].astype(BF16)

    def give_near(p, carry):
        remote(
            near_ret.at[block(p - far_blocks)], near_in.at[block(p - far_blocks)],
            ret_ss.at[1], ret_rs.at[1], "expert", source_at(p),
        ).start()
        return carry

    lax.fori_loop(far_blocks, experts - 1, give_near, 0)
    last_block = blocks(per_chunk - 1, 1)
    own_back = pltpu.make_async_copy(
        near_ret.at[last_block], near_in.at[last_block], local_sem.at[6]
    )
    own_back.start()

    def all_near_back():
        others = blocks(0, per_chunk - 1)
        return remote(
            near_ret.at[others], near_in.at[others], ret_ss.at[1], ret_rs.at[1], "expert",
            lax.rem(mine + 1, experts),
        )

    for j in range(done, messages):
        gather_step(exp_ring, j)

    def scatter_copy(refs, c, j, way):
        send, recv, send_sem, recv_sem = refs[1:]
        return remote(
            send.at[way, c, j], recv.at[way, c, j],
            send_sem.at[way, c, j], recv_sem.at[way, c, j], "mp", on_ring(1 - 2 * way),
        )

    def scatter_send(refs, c, j):
        part, send, recv = refs[:3]
        half = send.shape[3]
        for way in (0, 1):
            turn = 1 - 2 * way
            dest = on_ring(turn * (ring // 2 - (j + 1) // 2))
            start = pl.multiple_of(c * 2 * half + ((j + way) % 2) * half, half)
            value = part[dest, pl.ds(start, half), :]
            if j >= 2:
                scatter_copy(refs, c, j - 2, way).wait_recv()
                value = value + recv[way, c, j - 2].astype(F32)
            send[way, c, j] = value.astype(BF16)
            scatter_copy(refs, c, j, way).start()

    def scatter_sum(refs, c, h):
        part, send, recv = refs[:3]
        half = send.shape[3]
        start = pl.multiple_of(c * 2 * half + h * half, half)
        value = part[me, pl.ds(start, half), :]
        for way in (0, 1):
            j = messages - 1 if h == way else messages - 2
            scatter_copy(refs, c, j, way).wait_recv()
            value = value + recv[way, c, j].astype(F32)
        return value

    res_sums = (res_part, rs_send, rs_recv, rs_ss, rs_rs)
    exp_sums = (exp_part, es_send, es_recv, es_ss, es_rs)

    def expert(c, carry):
        rows, part = expert_rows(c)
        for k in range(ring):
            exp_part[k, rows, :] = part[:, k * width : (k + 1) * width]
        scatter_send(exp_sums, c, 0)
        scatter_send(exp_sums, c, 1)
        return carry

    lax.fori_loop(0, chunks - 1, expert, 0)

    def wave(j):
        def one(c, carry):
            scatter_send(exp_sums, c, j)
            return carry

        lax.fori_loop(0, chunks - 1, one, 0)

    wave(2)

    own_back.wait()
    all_near_back().wait_recv()
    near_rows = pl.ds(far_rows, chunk_rows)
    for tile in range(tiles):
        rows = pl.ds(tile * res_rows, res_rows)
        back = jnp.dot(table[rows, near_rows], near_in[...], preferred_element_type=F32)
        gates = gate_cols[rows, :]
        for k in range(ring):
            res_part[k, rows, :] += gates * back[:, k * width : (k + 1) * width]
    scatter_send(res_sums, 0, 0)
    scatter_send(res_sums, 0, 1)

    for j in range(3, messages):
        wave(j)
    early = min(4, messages)
    for j in range(2, early):
        scatter_send(res_sums, 0, j)

    def give_back(p, carry):
        remote(
            ret_send.at[block(p)], returned.at[block(p)],
            ret_ss.at[0], ret_rs.at[0], "expert", source_at(p),
        ).start()
        return carry

    half_rows = chunk_rows // 2
    for c in range(chunks - 1):
        for h in (0, 1):
            ret_send[pl.ds(c * chunk_rows + h * half_rows, half_rows), :] = scatter_sum(
                exp_sums, c, h
            ).astype(BF16)
        lax.fori_loop(c * per_chunk, (c + 1) * per_chunk, give_back, 0)

    for j in range(early, messages):
        scatter_send(res_sums, 0, j)

    def all_returned():
        return remote(
            ret_send.at[far], returned.at[far], ret_ss.at[0], ret_rs.at[0], "expert",
            lax.rem(mine + 1, experts),
        )

    all_returned().wait_recv()
    half = tokens // 2
    for h in (1, 0):
        rows = pl.ds(h * half, half)
        moe = jnp.dot(table[rows, pl.ds(0, far_rows)], returned[...], preferred_element_type=F32)
        gated = gate_cols[rows, :] * moe
        out[rows, :] = (scatter_sum(res_sums, 0, h) + gated).astype(BF16)

    all_dispatched().wait_send()
    all_near().wait_send()
    all_near_back().wait_send()
    all_returned().wait_send()
    for j in range(messages):
        for way in (0, 1):
            gather_copy(tok_ring, j, way, False).wait_send()
            gather_copy(exp_ring, j, way, False).wait_send()
            scatter_copy(res_sums, 0, j, way).wait_send()

    def drain(c, carry):
        for j in range(messages):
            for way in (0, 1):
                scatter_copy(exp_sums, c, j, way).wait_send()
        return carry

    lax.fori_loop(0, chunks - 1, drain, 0)


def per_device(
    experts, ring, tokens, gain, w_res_in, w_res_out, w_exp_in, w_exp_out,
    expert_of, slot_of, gate_prob,
):
    count, width = tokens.shape
    model, hidden = w_res_in.shape
    capacity = max(2, 5 * count // (4 * experts))
    slots = -(-capacity // 16) * 16
    chunks = 4 if experts % 8 == 0 else 2
    total = experts * slots
    messages = ring - 1
    near_rows = total // chunks
    far_rows = total - near_rows

    any_space = pl.BlockSpec(memory_space=pl.ANY)
    in_vmem = pl.BlockSpec(memory_space=pltpu.VMEM)
    sems = pltpu.SemaphoreType.DMA
    res_half, exp_half = count // 2, total // chunks // 2
    return pl.pallas_call(
        functools.partial(layer_kernel, experts, ring, slots, chunks),
        out_shape=jax.ShapeDtypeStruct((count, width), BF16),
        in_specs=[any_space] * 9,
        out_specs=in_vmem,
        scratch_shapes=[
            pltpu.VMEM((count // width, width), jnp.int32),
            pltpu.VMEM((count // width, width), jnp.int32),
            pltpu.VMEM((count // width, width), F32),
            pltpu.VMEM((1, model), F32),
            pltpu.VMEM((ring, count, width), BF16),
            pltpu.VMEM((ring, total, width), BF16),
            pltpu.VMEM((far_rows, width), BF16),
            pltpu.VMEM((ring, near_rows, width), BF16),
            pltpu.VMEM((model, hidden), BF16),
            pltpu.VMEM((hidden, model), BF16),
            pltpu.VMEM((model, hidden), BF16),
            pltpu.VMEM((hidden, model), BF16),
            pltpu.VMEM((ring, count, width), F32),
            pltpu.VMEM((ring, far_rows, width), F32),
            pltpu.VMEM((2, 1, messages, res_half, width), BF16),
            pltpu.VMEM((2, 1, messages, res_half, width), BF16),
            pltpu.VMEM((2, chunks - 1, messages, exp_half, width), BF16),
            pltpu.VMEM((2, chunks - 1, messages, exp_half, width), BF16),
            pltpu.VMEM((far_rows, width), BF16),
            pltpu.VMEM((far_rows, width), BF16),
            pltpu.VMEM((near_rows, model), BF16),
            pltpu.VMEM((near_rows, model), BF16),
            pltpu.VMEM((count, total), BF16),
            pltpu.VMEM((count, width), F32),
            sems((11,)),
            sems((2, messages)),
            sems((2, messages)),
            sems((2, messages)),
            sems((2, messages)),
            sems((2,)),
            sems((2,)),
            sems((2, 1, messages)),
            sems((2, 1, messages)),
            sems((2, chunks - 1, messages)),
            sems((2, chunks - 1, messages)),
            sems((2,)),
            sems((2,)),
        ],
        compiler_params=pltpu.CompilerParams(
            collective_id=0, has_side_effects=True, vmem_limit_bytes=56 * 1024 * 1024
        ),
        name="moe_layer",
    )(
        expert_of.reshape(-1, width), slot_of.reshape(-1, width), gate_prob.reshape(-1, width),
        gain.reshape(1, model), tokens, w_res_in, w_res_out, w_exp_in[0], w_exp_out[0],
    )


def solution(mesh):
    return jax.shard_map(
        functools.partial(per_device, mesh.shape["expert"], mesh.shape["mp"]),
        mesh=mesh,
        in_specs=(
            P(("groups", "expert"), "mp"),
            P(),
            P(None, "mp"),
            P("mp", None),
            P("expert", None, "mp"),
            P("expert", "mp", None),
            P(("groups", "expert")),
            P(("groups", "expert")),
            P(("groups", "expert")),
        ),
        out_specs=P(("groups", "expert"), "mp"),
        check_vma=False,
    )
```

```python
import functools

import jax
import jax.numpy as jnp
from jax import lax
from jax.experimental import pallas as pl
from jax.experimental.pallas import tpu as pltpu
from jax.sharding import PartitionSpec as P

MESH = pl.DeviceIdType.MESH
BF16 = jnp.bfloat16
F32 = jnp.float32


def rms_rows(pieces, gain):
    values = jnp.concatenate([piece.astype(F32) for piece in pieces], axis=1)
    inverse = lax.rsqrt(jnp.mean(values * values, axis=-1, keepdims=True) + 1e-05)
    return (values * inverse * gain).astype(BF16)


def mlp_rows(rows, w_in, w_out):
    hidden = jax.nn.gelu(jnp.dot(rows, w_in[...], preferred_element_type=F32)).astype(BF16)
    return jnp.dot(hidden, w_out[...], preferred_element_type=F32)


def remote(src, dst, send_sem, recv_sem, axis, device):
    return pltpu.make_async_remote_copy(
        src_ref=src,
        dst_ref=dst,
        send_sem=send_sem,
        recv_sem=recv_sem,
        device_id={axis: device},
        device_id_type=MESH,
    )


def layer_kernel(
    experts, ring, slots, chunks,
    ids_hbm, slots_hbm, gate_hbm, gain_hbm, tok_hbm, wri_hbm, wro_hbm, wei_hbm, weo_hbm, out,
    ids, slot, gate, gain_row, tok_all, exp_all, outgoing, near_out, wri, wro, wei, weo,
    res_part, exp_part, rs_send, rs_recv, es_send, es_recv, ret_send, returned,
    near_ret, near_in, table, gate_cols,
    local_sem, tok_ss, tok_rs, exp_ss, exp_rs, dis_ss, dis_rs,
    rs_ss, rs_rs, es_ss, es_rs, ret_ss, ret_rs,
):
    me = lax.axis_index("mp")
    mine = lax.axis_index("expert")
    tokens, width = out.shape
    total = experts * slots
    messages = ring - 1
    chunk_rows = total // chunks
    per_chunk = experts // chunks
    near_blocks = per_chunk
    mid_blocks = per_chunk // 2
    far_blocks = experts - near_blocks
    ring_blocks = far_blocks - mid_blocks
    far_rows = far_blocks * slots
    ring_rows = ring_blocks * slots

    def on_ring(offset):
        return lax.rem(me + offset + 2 * ring, ring)

    def partner(p):
        far = lax.div(p + 1, 2)
        return experts // 2 + jnp.where(lax.rem(p, 2) == 0, far, -far)

    def expert_at(p):
        return lax.rem(mine - partner(p) + experts, experts)

    def source_at(p):
        return lax.rem(mine + partner(p), experts)

    def block(at):
        return pl.ds(pl.multiple_of(at * slots, slots), slots)

    def blocks(first, count):
        return pl.ds(first * slots, count * slots)

    tok_copy = pltpu.make_async_copy(tok_hbm, tok_all.at[me], local_sem.at[0])
    tok_copy.start()

    barrier = pltpu.get_barrier_semaphore()
    for offset in (-1, 1):
        pl.semaphore_signal(
            barrier, inc=1, device_id={"mp": on_ring(offset)}, device_id_type=MESH
        )

    def greet(step, carry):
        pl.semaphore_signal(
            barrier,
            inc=1,
            device_id={"expert": lax.rem(mine + step, experts)},
            device_id_type=MESH,
        )
        return carry

    lax.fori_loop(1, experts, greet, 0)

    small_copies = [
        pltpu.make_async_copy(src, dst, local_sem.at[7 + at])
        for at, (src, dst) in enumerate(
            ((ids_hbm, ids), (slots_hbm, slot), (gate_hbm, gate), (gain_hbm, gain_row))
        )
    ]
    for copy in small_copies:
        copy.start()
    weight_copies = [
        pltpu.make_async_copy(src, dst, local_sem.at[1 + at])
        for at, (src, dst) in enumerate(
            ((wri_hbm, wri), (wro_hbm, wro), (wei_hbm, wei), (weo_hbm, weo))
        )
    ]
    for copy in weight_copies:
        copy.start()
    for copy in small_copies:
        copy.wait()
    tok_copy.wait()
    pl.semaphore_wait(barrier, experts + 1)

    def gather_copy(refs, j, way, arriving):
        buf, rows, send_sem, recv_sem = refs
        turn = 1 - 2 * way
        half = rows // 2
        shard = on_ring(-turn * (j // 2 + (1 if arriving else 0)))
        ref = buf.at[shard, pl.ds(((j + way) % 2) * half, half)]
        return remote(ref, ref, send_sem.at[way, j], recv_sem.at[way, j], "mp", on_ring(turn))

    def gather_send(refs, j):
        for way in (0, 1):
            gather_copy(refs, j, way, False).start()

    def gather_step(refs, j):
        for way in (0, 1):
            gather_copy(refs, j, way, True).wait_recv()
            if j + 2 < messages:
                gather_copy(refs, j + 2, way, False).start()

    tok_ring = (tok_all, tokens, tok_ss, tok_rs)
    exp_ring = (exp_all, ring_rows, exp_ss, exp_rs)
    gather_send(tok_ring, 0)
    gather_send(tok_ring, 1)

    def as_row(values):
        return jnp.concatenate([values[at : at + 1] for at in range(values.shape[0])], axis=1)

    slot_row = as_row(jnp.where(slot[...] >= 0, ids[...] * slots + slot[...], -1))

    def send_hits(first, count):
        step = lax.broadcasted_iota(jnp.int32, (slots, tokens), 0)
        hits = [
            jnp.where(step + expert_at(first + at) * slots == slot_row, 1.0, 0.0)
            for at in range(count)
        ]
        return jnp.concatenate(hits, axis=0).astype(BF16)

    def dispatch(p, carry):
        remote(
            outgoing.at[block(p)], exp_all.at[me, block(p)],
            dis_ss.at[0], dis_rs.at[0], "expert", expert_at(p),
        ).start()
        return carry

    group = mid_blocks

    def pick(c, carry):
        rows = pl.ds(pl.multiple_of(c * group * slots, slots), group * slots)
        outgoing[rows, :] = jnp.dot(
            send_hits(c * group, group), tok_all[me], preferred_element_type=F32
        ).astype(BF16)
        return lax.fori_loop(c * group, (c + 1) * group, dispatch, carry)

    lax.fori_loop(0, ring_blocks // group, pick, 0)

    def turned(row):
        return jnp.transpose(jnp.broadcast_to(row, (width, tokens)))

    gate_cols[...] = turned(as_row(gate[...]))
    slot_cols = turned(slot_row.astype(F32))
    lane = lax.broadcasted_iota(jnp.int32, (1, total), 1)
    wanted = jnp.zeros((1, total), jnp.int32)
    for p in range(experts):
        inside = jnp.logical_and(lane >= p * slots, lane < (p + 1) * slots)
        wanted = jnp.where(inside, lane + (expert_at(p) - p) * slots, wanted)
    wanted = wanted.astype(F32)
    for at in range(0, total, width):
        wide = min(width, total - at)
        hit = jnp.where(slot_cols[:, :wide] == wanted[:, at : at + wide], 1.0, 0.0)
        table[:, at : at + wide] = hit.astype(BF16)

    for j in range(messages - 2):
        gather_step(tok_ring, j)

    anyone = lax.rem(mine + 1, experts)
    far = blocks(0, far_blocks)
    ringed = blocks(0, ring_blocks)

    def all_dispatched():
        return remote(
            outgoing.at[ringed], exp_all.at[me, ringed], dis_ss.at[0], dis_rs.at[0], "expert", anyone,
        )

    all_dispatched().wait_recv()
    gather_send(exp_ring, 0)
    gather_send(exp_ring, 1)
    for j in range(messages - 2, messages):
        gather_step(tok_ring, j)

    def whole_copy(first, count, sem, target):
        return remote(
            near_out.at[:, pl.ds(pl.multiple_of((first - ring_blocks) * slots, slots), count * slots), :],
            exp_all.at[:, pl.ds(pl.multiple_of(first * slots, slots), count * slots), :],
            dis_ss.at[sem], dis_rs.at[sem], "expert", target,
        )

    def dispatch_whole(first, count, last, sem):
        hits = send_hits(first, count)
        rows = pl.ds((first - ring_blocks) * slots, count * slots)
        for k in range(ring):
            near_out[k, rows, :] = jnp.dot(
                hits, tok_all[k], preferred_element_type=F32
            ).astype(BF16)

        def one(p, carry):
            whole_copy(p, 1, sem, expert_at(p)).start()
            return carry

        lax.fori_loop(first, last, one, 0)

    dispatch_whole(far_blocks, near_blocks, experts - 1, 1)
    own_copy = pltpu.make_async_copy(
        near_out.at[:, blocks(experts - 1 - ring_blocks, 1), :],
        exp_all.at[:, blocks(experts - 1, 1), :],
        local_sem.at[5],
    )
    own_copy.start()
    dispatch_whole(ring_blocks, mid_blocks, far_blocks, 2)

    def all_near():
        return whole_copy(far_blocks, near_blocks - 1, 1, anyone)

    def all_mid():
        return whole_copy(ring_blocks, mid_blocks, 2, anyone)

    gain = gain_row[...]
    weight_copies[0].wait()
    weight_copies[1].wait()
    tiles = 3 if tokens % 48 == 0 else 1
    res_rows = tokens // tiles
    for tile in range(tiles):
        rows = pl.ds(tile * res_rows, res_rows)
        normed = rms_rows([tok_all[k, rows, :] for k in range(ring)], gain)
        part = mlp_rows(normed, wri, wro)
        for k in range(ring):
            res_part[k, rows, :] = part[:, k * width : (k + 1) * width]
        if tile < messages - 3:
            gather_step(exp_ring, tile)
    done = min(tiles, messages - 3)

    def expert_rows(c):
        rows = pl.ds(pl.multiple_of(c * chunk_rows, chunk_rows), chunk_rows)
        normed = rms_rows([exp_all[k, rows, :] for k in range(ring)], gain)
        return rows, mlp_rows(normed, wei, weo)

    weight_copies[2].wait()
    weight_copies[3].wait()
    own_copy.wait()
    all_near().wait_recv()
    near_ret[...] = expert_rows(chunks - 1)[1].astype(BF16)

    def give_near(p, carry):
        remote(
            near_ret.at[block(p - far_blocks)], near_in.at[block(p - far_blocks)],
            ret_ss.at[1], ret_rs.at[1], "expert", source_at(p),
        ).start()
        return carry

    lax.fori_loop(far_blocks, experts - 1, give_near, 0)
    last_block = blocks(per_chunk - 1, 1)
    own_back = pltpu.make_async_copy(
        near_ret.at[last_block], near_in.at[last_block], local_sem.at[6]
    )
    own_back.start()

    def all_near_back():
        others = blocks(0, near_blocks - 1)
        return remote(
            near_ret.at[others], near_in.at[others], ret_ss.at[1], ret_rs.at[1], "expert", anyone,
        )

    for j in range(done, messages):
        gather_step(exp_ring, j)

    def scatter_copy(refs, c, j, way):
        send, recv, send_sem, recv_sem = refs[1:]
        return remote(
            send.at[way, c, j], recv.at[way, c, j],
            send_sem.at[way, c, j], recv_sem.at[way, c, j], "mp", on_ring(1 - 2 * way),
        )

    def scatter_send(refs, c, j):
        part, send, recv = refs[:3]
        half = send.shape[3]
        for way in (0, 1):
            turn = 1 - 2 * way
            dest = on_ring(turn * (ring // 2 - (j + 1) // 2))
            start = pl.multiple_of(c * 2 * half + ((j + way) % 2) * half, half)
            value = part[dest, pl.ds(start, half), :]
            if j >= 2:
                scatter_copy(refs, c, j - 2, way).wait_recv()
                value = value + recv[way, c, j - 2].astype(F32)
            send[way, c, j] = value.astype(BF16)
            scatter_copy(refs, c, j, way).start()

    def scatter_sum(refs, c, h):
        part, send, recv = refs[:3]
        half = send.shape[3]
        start = pl.multiple_of(c * 2 * half + h * half, half)
        value = part[me, pl.ds(start, half), :]
        for way in (0, 1):
            j = messages - 1 if h == way else messages - 2
            scatter_copy(refs, c, j, way).wait_recv()
            value = value + recv[way, c, j].astype(F32)
        return value

    res_sums = (res_part, rs_send, rs_recv, rs_ss, rs_rs)
    exp_sums = (exp_part, es_send, es_recv, es_ss, es_rs)

    def expert(c):
        rows, part = expert_rows(c)
        for k in range(ring):
            exp_part[k, rows, :] = part[:, k * width : (k + 1) * width]

    def merge():
        own_back.wait()
        all_near_back().wait_recv()
        near_rows = pl.ds(far_rows, chunk_rows)
        for tile in range(tiles):
            rows = pl.ds(tile * res_rows, res_rows)
            back = jnp.dot(table[rows, near_rows], near_in[...], preferred_element_type=F32)
            gates = gate_cols[rows, :]
            for k in range(ring):
                res_part[k, rows, :] += gates * back[:, k * width : (k + 1) * width]

    def give_back(p, carry):
        remote(
            ret_send.at[block(p)], returned.at[block(p)],
            ret_ss.at[0], ret_rs.at[0], "expert", source_at(p),
        ).start()
        return carry

    half_rows = chunk_rows // 2

    def finish(c):
        for h in (0, 1):
            ret_send[pl.ds(c * chunk_rows + h * half_rows, half_rows), :] = scatter_sum(
                exp_sums, c, h
            ).astype(BF16)
        lax.fori_loop(c * per_chunk, (c + 1) * per_chunk, give_back, 0)

    def term(c, *steps):
        for j in steps:
            if j < messages:
                scatter_send(exp_sums, c, j)

    def res_term(*steps):
        for j in steps:
            if j < messages:
                scatter_send(res_sums, 0, j)

    expert(0)
    term(0, 0, 1)
    expert(1)
    term(1, 0, 1)
    all_mid().wait_recv()
    expert(2)
    term(0, 2, 3)
    term(2, 0, 1)
    term(0, 4, 5)
    term(1, 2, 3)
    term(0, 6)
    term(2, 2, 3)
    merge()
    term(1, 4, 5)
    finish(0)
    res_term(0)
    term(2, 4, 5)
    term(1, 6)
    term(2, 6)
    res_term(1)
    finish(1)
    finish(2)
    res_term(2, 3, 4, 5, 6)

    def all_returned():
        return remote(
            ret_send.at[far], returned.at[far], ret_ss.at[0], ret_rs.at[0], "expert", anyone,
        )

    all_returned().wait_recv()
    half = tokens // 2
    halves = [pl.ds(h * half, half) for h in (0, 1)]
    gated = [
        gate_cols[rows, :]
        * jnp.dot(table[rows, pl.ds(0, far_rows)], returned[...], preferred_element_type=F32)
        for rows in halves
    ]
    for h, rows in enumerate(halves):
        out[rows, :] = scatter_sum(res_sums, 0, h) + gated[h]

    all_dispatched().wait_send()
    all_near().wait_send()
    all_mid().wait_send()
    all_near_back().wait_send()
    all_returned().wait_send()
    for j in range(messages):
        for way in (0, 1):
            gather_copy(tok_ring, j, way, False).wait_send()
            gather_copy(exp_ring, j, way, False).wait_send()
            scatter_copy(res_sums, 0, j, way).wait_send()

    def drain(c, carry):
        for j in range(messages):
            for way in (0, 1):
                scatter_copy(exp_sums, c, j, way).wait_send()
        return carry

    lax.fori_loop(0, chunks - 1, drain, 0)


def per_device(
    experts, ring, tokens, gain, w_res_in, w_res_out, w_exp_in, w_exp_out,
    expert_of, slot_of, gate_prob,
):
    count, width = tokens.shape
    model, hidden = w_res_in.shape
    capacity = max(2, 5 * count // (4 * experts))
    slots = -(-capacity // 16) * 16
    chunks = 4 if experts % 8 == 0 else 2
    total = experts * slots
    messages = ring - 1
    near_rows = total // chunks
    far_rows = total - near_rows
    ring_rows = far_rows - near_rows // 2

    any_space = pl.BlockSpec(memory_space=pl.ANY)
    in_vmem = pl.BlockSpec(memory_space=pltpu.VMEM)
    sems = pltpu.SemaphoreType.DMA
    res_half, exp_half = count // 2, total // chunks // 2
    return pl.pallas_call(
        functools.partial(layer_kernel, experts, ring, slots, chunks),
        out_shape=jax.ShapeDtypeStruct((count, width), F32),
        in_specs=[any_space] * 9,
        out_specs=in_vmem,
        scratch_shapes=[
            pltpu.VMEM((count // width, width), jnp.int32),
            pltpu.VMEM((count // width, width), jnp.int32),
            pltpu.VMEM((count // width, width), F32),
            pltpu.VMEM((1, model), F32),
            pltpu.VMEM((ring, count, width), BF16),
            pltpu.VMEM((ring, total, width), BF16),
            pltpu.VMEM((ring_rows, width), BF16),
            pltpu.VMEM((ring, total - ring_rows, width), BF16),
            pltpu.VMEM((model, hidden), BF16),
            pltpu.VMEM((hidden, model), BF16),
            pltpu.VMEM((model, hidden), BF16),
            pltpu.VMEM((hidden, model), BF16),
            pltpu.VMEM((ring, count, width), F32),
            pltpu.VMEM((ring, far_rows, width), F32),
            pltpu.VMEM((2, 1, messages, res_half, width), BF16),
            pltpu.VMEM((2, 1, messages, res_half, width), BF16),
            pltpu.VMEM((2, chunks - 1, messages, exp_half, width), BF16),
            pltpu.VMEM((2, chunks - 1, messages, exp_half, width), BF16),
            pltpu.VMEM((far_rows, width), BF16),
            pltpu.VMEM((far_rows, width), BF16),
            pltpu.VMEM((near_rows, model), BF16),
            pltpu.VMEM((near_rows, model), BF16),
            pltpu.VMEM((count, total), BF16),
            pltpu.VMEM((count, width), F32),
            sems((11,)),
            sems((2, messages)),
            sems((2, messages)),
            sems((2, messages)),
            sems((2, messages)),
            sems((3,)),
            sems((3,)),
            sems((2, 1, messages)),
            sems((2, 1, messages)),
            sems((2, chunks - 1, messages)),
            sems((2, chunks - 1, messages)),
            sems((2,)),
            sems((2,)),
        ],
        compiler_params=pltpu.CompilerParams(
            collective_id=0, has_side_effects=True, vmem_limit_bytes=56 * 1024 * 1024
        ),
        name="moe_layer",
    )(
        expert_of.reshape(-1, width), slot_of.reshape(-1, width), gate_prob.reshape(-1, width),
        gain.reshape(1, model), tokens, w_res_in, w_res_out, w_exp_in[0], w_exp_out[0],
    ).astype(BF16)


def solution(mesh):
    return jax.shard_map(
        functools.partial(per_device, mesh.shape["expert"], mesh.shape["mp"]),
        mesh=mesh,
        in_specs=(
            P(("groups", "expert"), "mp"),
            P(),
            P(None, "mp"),
            P("mp", None),
            P("expert", None, "mp"),
            P("expert", "mp", None),
            P(("groups", "expert")),
            P(("groups", "expert")),
            P(("groups", "expert")),
        ),
        out_specs=P(("groups", "expert"), "mp"),
        check_vma=False,
    )
```

```python
import functools

import jax
import jax.numpy as jnp
from jax import lax
from jax.experimental import pallas as pl
from jax.experimental.pallas import tpu as pltpu
from jax.sharding import PartitionSpec as P

MESH = pl.DeviceIdType.MESH
BF16 = jnp.bfloat16
F32 = jnp.float32


def rms_rows(pieces, gain):
    values = jnp.concatenate([piece.astype(F32) for piece in pieces], axis=1)
    inverse = lax.rsqrt(jnp.mean(values * values, axis=-1, keepdims=True) + 1e-05)
    return (values * inverse * gain).astype(BF16)


def mlp_rows(rows, w_in, w_out):
    hidden = jax.nn.gelu(jnp.dot(rows, w_in[...], preferred_element_type=F32)).astype(BF16)
    return jnp.dot(hidden, w_out[...], preferred_element_type=F32)


def remote(src, dst, send_sem, recv_sem, axis, device):
    return pltpu.make_async_remote_copy(
        src_ref=src,
        dst_ref=dst,
        send_sem=send_sem,
        recv_sem=recv_sem,
        device_id={axis: device},
        device_id_type=MESH,
    )


def layer_kernel(
    experts, ring, slots, chunks, tiles, pieces,
    ids_hbm, slots_hbm, gate_hbm, gain_hbm, tok_hbm, wri_hbm, wro_hbm, wei_hbm, weo_hbm, out,
    ids, slot, gate, gain_row, tok_all, exp_all, outgoing, near_out, wri, wro, wei, weo,
    res_part, exp_part, rs_send, rs_recv, es_send, es_recv, ret_send, returned,
    near_ret, near_in, table, gate_cols,
    local_sem, tok_ss, tok_rs, exp_ss, exp_rs, dis_ss, dis_rs,
    rs_ss, rs_rs, es_ss, es_rs, ret_ss, ret_rs,
):
    me = lax.axis_index("mp")
    mine = lax.axis_index("expert")
    tokens, width = out.shape
    total = experts * slots
    messages = ring - 1
    chunk_rows = total // chunks
    per_chunk = experts // chunks
    near_blocks = per_chunk
    mid_blocks = per_chunk // 2
    far_blocks = experts - near_blocks
    ring_blocks = far_blocks - mid_blocks
    far_rows = far_blocks * slots
    ring_rows = ring_blocks * slots

    def on_ring(offset):
        return lax.rem(me + offset + 2 * ring, ring)

    def partner(p):
        far = lax.div(p + 1, 2)
        return experts // 2 + jnp.where(lax.rem(p, 2) == 0, far, -far)

    def expert_at(p):
        return lax.rem(mine - partner(p) + experts, experts)

    def source_at(p):
        return lax.rem(mine + partner(p), experts)

    def block(at):
        return pl.ds(pl.multiple_of(at * slots, slots), slots)

    def blocks(first, count):
        return pl.ds(first * slots, count * slots)

    tok_copy = pltpu.make_async_copy(tok_hbm, tok_all.at[me], local_sem.at[0])
    tok_copy.start()

    barrier = pltpu.get_barrier_semaphore()
    for offset in (-1, 1):
        pl.semaphore_signal(
            barrier, inc=1, device_id={"mp": on_ring(offset)}, device_id_type=MESH
        )

    def greet(step, carry):
        pl.semaphore_signal(
            barrier,
            inc=1,
            device_id={"expert": lax.rem(mine + step, experts)},
            device_id_type=MESH,
        )
        return carry

    lax.fori_loop(1, experts, greet, 0)

    small_copies = [
        pltpu.make_async_copy(src, dst, local_sem.at[7 + at])
        for at, (src, dst) in enumerate(
            ((ids_hbm, ids), (slots_hbm, slot), (gate_hbm, gate), (gain_hbm, gain_row))
        )
    ]
    for copy in small_copies:
        copy.start()
    weight_copies = [
        pltpu.make_async_copy(src, dst, local_sem.at[1 + at])
        for at, (src, dst) in enumerate(
            ((wri_hbm, wri), (wro_hbm, wro), (wei_hbm, wei), (weo_hbm, weo))
        )
    ]
    for copy in weight_copies:
        copy.start()
    for copy in small_copies:
        copy.wait()
    tok_copy.wait()
    pl.semaphore_wait(barrier, experts + 1)

    gathered = messages * pieces // 2

    def gather_copy(refs, j, way, arriving):
        buf, rows, send_sem, recv_sem = refs
        turn = 1 - 2 * way
        size = rows // pieces
        shard = on_ring(-turn * (j // pieces + (1 if arriving else 0)))
        piece = (j + way * (pieces // 2)) % pieces
        ref = buf.at[shard, pl.ds(piece * size, size)]
        return remote(ref, ref, send_sem.at[way, j], recv_sem.at[way, j], "mp", on_ring(turn))

    def gather_send(refs):
        for j in range(pieces):
            for way in (0, 1):
                gather_copy(refs, j, way, False).start()

    def gather_step(refs, j):
        for way in (0, 1):
            gather_copy(refs, j, way, True).wait_recv()
            if j + pieces < gathered:
                gather_copy(refs, j + pieces, way, False).start()

    tok_ring = (tok_all, tokens, tok_ss, tok_rs)
    exp_ring = (exp_all, ring_rows, exp_ss, exp_rs)
    gather_send(tok_ring)

    def as_row(values):
        return jnp.concatenate([values[at : at + 1] for at in range(values.shape[0])], axis=1)

    slot_row = as_row(jnp.where(slot[...] >= 0, ids[...] * slots + slot[...], -1))

    def send_hits(first, count):
        step = lax.broadcasted_iota(jnp.int32, (slots, tokens), 0)
        hits = [
            jnp.where(step + expert_at(first + at) * slots == slot_row, 1.0, 0.0)
            for at in range(count)
        ]
        return jnp.concatenate(hits, axis=0).astype(BF16)

    def dispatch(p, carry):
        remote(
            outgoing.at[block(p)], exp_all.at[me, block(p)],
            dis_ss.at[0], dis_rs.at[0], "expert", expert_at(p),
        ).start()
        return carry

    group = mid_blocks

    def pick(c, carry):
        rows = pl.ds(pl.multiple_of(c * group * slots, slots), group * slots)
        outgoing[rows, :] = jnp.dot(
            send_hits(c * group, group), tok_all[me], preferred_element_type=F32
        ).astype(BF16)
        return lax.fori_loop(c * group, (c + 1) * group, dispatch, carry)

    lax.fori_loop(0, ring_blocks // group, pick, 0)

    def turned(row):
        return jnp.transpose(jnp.broadcast_to(row, (width, tokens)))

    gate_cols[...] = turned(as_row(gate[...]))
    slot_cols = turned(slot_row.astype(F32))
    lane = lax.broadcasted_iota(jnp.int32, (1, total), 1)
    wanted = jnp.zeros((1, total), jnp.int32)
    for p in range(experts):
        inside = jnp.logical_and(lane >= p * slots, lane < (p + 1) * slots)
        wanted = jnp.where(inside, lane + (expert_at(p) - p) * slots, wanted)
    wanted = wanted.astype(F32)
    for at in range(0, total, width):
        wide = min(width, total - at)
        hit = jnp.where(slot_cols[:, :wide] == wanted[:, at : at + wide], 1.0, 0.0)
        table[:, at : at + wide] = hit.astype(BF16)

    for j in range(gathered - pieces):
        gather_step(tok_ring, j)

    anyone = lax.rem(mine + 1, experts)
    far = blocks(0, far_blocks)
    ringed = blocks(0, ring_blocks)

    def all_dispatched():
        return remote(
            outgoing.at[ringed], exp_all.at[me, ringed], dis_ss.at[0], dis_rs.at[0], "expert", anyone,
        )

    all_dispatched().wait_recv()
    gather_send(exp_ring)
    for j in range(gathered - pieces, gathered):
        gather_step(tok_ring, j)

    def whole_copy(first, count, sem, target):
        return remote(
            near_out.at[:, pl.ds(pl.multiple_of((first - ring_blocks) * slots, slots), count * slots), :],
            exp_all.at[:, pl.ds(pl.multiple_of(first * slots, slots), count * slots), :],
            dis_ss.at[sem], dis_rs.at[sem], "expert", target,
        )

    def dispatch_whole(first, count, last, sem):
        hits = send_hits(first, count)
        rows = pl.ds((first - ring_blocks) * slots, count * slots)
        for k in range(ring):
            near_out[k, rows, :] = jnp.dot(
                hits, tok_all[k], preferred_element_type=F32
            ).astype(BF16)

        def one(p, carry):
            whole_copy(p, 1, sem, expert_at(p)).start()
            return carry

        lax.fori_loop(first, last, one, 0)

    dispatch_whole(far_blocks, near_blocks, experts - 1, 1)
    own_copy = pltpu.make_async_copy(
        near_out.at[:, blocks(experts - 1 - ring_blocks, 1), :],
        exp_all.at[:, blocks(experts - 1, 1), :],
        local_sem.at[5],
    )
    own_copy.start()
    exp_steps = iter(range(gathered))

    def exp_advance(count):
        for j in range(count):
            gather_step(exp_ring, next(exp_steps))

    exp_advance(1)
    dispatch_whole(ring_blocks, mid_blocks, far_blocks, 2)

    def all_near():
        return whole_copy(far_blocks, near_blocks - 1, 1, anyone)

    def all_mid():
        return whole_copy(ring_blocks, mid_blocks, 2, anyone)

    gain = gain_row[...]
    weight_copies[0].wait()
    weight_copies[1].wait()
    res_rows = tokens // tiles
    relayed = gathered - pieces
    for tile in range(tiles):
        exp_advance((relayed - 1) // (tiles + 1))
        rows = pl.ds(tile * res_rows, res_rows)
        normed = rms_rows([tok_all[k, rows, :] for k in range(ring)], gain)
        part = mlp_rows(normed, wri, wro)
        for k in range(ring):
            res_part[k, rows, :] = part[:, k * width : (k + 1) * width]
    exp_advance(relayed - 1 - tiles * ((relayed - 1) // (tiles + 1)))

    def expert_rows(c):
        rows = pl.ds(pl.multiple_of(c * chunk_rows, chunk_rows), chunk_rows)
        normed = rms_rows([exp_all[k, rows, :] for k in range(ring)], gain)
        return rows, mlp_rows(normed, wei, weo)

    weight_copies[2].wait()
    weight_copies[3].wait()
    own_copy.wait()
    all_near().wait_recv()
    near_ret[...] = expert_rows(chunks - 1)[1].astype(BF16)

    def give_near(p, carry):
        remote(
            near_ret.at[block(p - far_blocks)], near_in.at[block(p - far_blocks)],
            ret_ss.at[1], ret_rs.at[1], "expert", source_at(p),
        ).start()
        return carry

    lax.fori_loop(far_blocks, experts - 1, give_near, 0)
    last_block = blocks(per_chunk - 1, 1)
    own_back = pltpu.make_async_copy(
        near_ret.at[last_block], near_in.at[last_block], local_sem.at[6]
    )
    own_back.start()

    def all_near_back():
        others = blocks(0, near_blocks - 1)
        return remote(
            near_ret.at[others], near_in.at[others], ret_ss.at[1], ret_rs.at[1], "expert", anyone,
        )

    exp_advance(pieces)

    def scatter_copy(refs, c, j, way):
        send, recv, send_sem, recv_sem = refs[1:]
        return remote(
            send.at[way, c, j], recv.at[way, c, j],
            send_sem.at[way, c, j], recv_sem.at[way, c, j], "mp", on_ring(1 - 2 * way),
        )

    def scatter_send(refs, c, j):
        part, send, recv = refs[:3]
        half = send.shape[3]
        for way in (0, 1):
            turn = 1 - 2 * way
            dest = on_ring(turn * (ring // 2 - (j + 1) // 2))
            start = pl.multiple_of(c * 2 * half + ((j + way) % 2) * half, half)
            value = part[dest, pl.ds(start, half), :]
            if j >= 2:
                scatter_copy(refs, c, j - 2, way).wait_recv()
                value = value + recv[way, c, j - 2].astype(F32)
            send[way, c, j] = value.astype(BF16)
            scatter_copy(refs, c, j, way).start()

    def scatter_sum(refs, c, h):
        part, send, recv = refs[:3]
        half = send.shape[3]
        start = pl.multiple_of(c * 2 * half + h * half, half)
        value = part[me, pl.ds(start, half), :]
        for way in (0, 1):
            j = messages - 1 if h == way else messages - 2
            scatter_copy(refs, c, j, way).wait_recv()
            value = value + recv[way, c, j].astype(F32)
        return value

    res_sums = (res_part, rs_send, rs_recv, rs_ss, rs_rs)
    exp_sums = (exp_part, es_send, es_recv, es_ss, es_rs)

    def expert(c):
        rows, part = expert_rows(c)
        for k in range(ring):
            exp_part[k, rows, :] = part[:, k * width : (k + 1) * width]

    def merge():
        own_back.wait()
        all_near_back().wait_recv()
        near_rows = pl.ds(far_rows, chunk_rows)
        for tile in range(tiles):
            rows = pl.ds(tile * res_rows, res_rows)
            back = jnp.dot(table[rows, near_rows], near_in[...], preferred_element_type=F32)
            gates = gate_cols[rows, :]
            for k in range(ring):
                res_part[k, rows, :] += gates * back[:, k * width : (k + 1) * width]

    def give_back(p, carry):
        remote(
            ret_send.at[block(p)], returned.at[block(p)],
            ret_ss.at[0], ret_rs.at[0], "expert", source_at(p),
        ).start()
        return carry

    half_rows = chunk_rows // 2

    def finish(c):
        for h in (0, 1):
            ret_send[pl.ds(c * chunk_rows + h * half_rows, half_rows), :] = scatter_sum(
                exp_sums, c, h
            ).astype(BF16)
        lax.fori_loop(c * per_chunk, (c + 1) * per_chunk, give_back, 0)

    def wave(refs, count, *steps):
        def one(c, carry, j=0):
            scatter_send(refs, c, j)
            return carry

        for j in steps:
            if j < messages:
                lax.fori_loop(0, count, functools.partial(one, j=j), 0)

    def exp_wave(*steps):
        wave(exp_sums, chunks - 1, *steps)

    def res_wave(*steps):
        wave(res_sums, tiles, *steps)

    for c in range(chunks - 1):
        if c == chunks - 2:
            all_mid().wait_recv()
        expert(c)
        scatter_send(exp_sums, c, 0)
        scatter_send(exp_sums, c, 1)
    exp_wave(2)
    merge()
    res_wave(0)
    exp_wave(3, 4)
    res_wave(1)
    exp_wave(5, 6)
    res_wave(2)
    for c in range(chunks - 1):
        finish(c)
    res_wave(3, 4, 5, 6)

    def all_returned():
        return remote(
            ret_send.at[far], returned.at[far], ret_ss.at[0], ret_rs.at[0], "expert", anyone,
        )

    all_returned().wait_recv()
    half = res_rows // 2
    parts = [pl.ds(at * half, half) for at in range(2 * tiles)]
    gated = [
        gate_cols[rows, :]
        * jnp.dot(table[rows, pl.ds(0, far_rows)], returned[...], preferred_element_type=F32)
        for rows in parts
    ]
    for at, rows in enumerate(parts):
        out[rows, :] = scatter_sum(res_sums, at // 2, at % 2) + gated[at]

    all_dispatched().wait_send()
    all_near().wait_send()
    all_mid().wait_send()
    all_near_back().wait_send()
    all_returned().wait_send()
    for j in range(gathered):
        for way in (0, 1):
            gather_copy(tok_ring, j, way, False).wait_send()
            gather_copy(exp_ring, j, way, False).wait_send()

    def drain(refs, c, carry):
        for j in range(messages):
            for way in (0, 1):
                scatter_copy(refs, c, j, way).wait_send()
        return carry

    lax.fori_loop(0, tiles, functools.partial(drain, res_sums), 0)
    lax.fori_loop(0, chunks - 1, functools.partial(drain, exp_sums), 0)


def per_device(
    experts, ring, tokens, gain, w_res_in, w_res_out, w_exp_in, w_exp_out,
    expert_of, slot_of, gate_prob,
):
    count, width = tokens.shape
    model, hidden = w_res_in.shape
    capacity = max(2, 5 * count // (4 * experts))
    slots = -(-capacity // 16) * 16
    chunks = 4 if experts % 8 == 0 else 2
    total = experts * slots
    messages = ring - 1
    near_rows = total // chunks
    far_rows = total - near_rows
    ring_rows = far_rows - near_rows // 2

    any_space = pl.BlockSpec(memory_space=pl.ANY)
    in_vmem = pl.BlockSpec(memory_space=pltpu.VMEM)
    sems = pltpu.SemaphoreType.DMA
    tiles = 3 if count % 96 == 0 else 1
    pieces = 4
    gathered = messages * pieces // 2
    res_half, exp_half = count // tiles // 2, total // chunks // 2
    return pl.pallas_call(
        functools.partial(layer_kernel, experts, ring, slots, chunks, tiles, pieces),
        out_shape=jax.ShapeDtypeStruct((count, width), F32),
        in_specs=[any_space] * 9,
        out_specs=in_vmem,
        scratch_shapes=[
            pltpu.VMEM((count // width, width), jnp.int32),
            pltpu.VMEM((count // width, width), jnp.int32),
            pltpu.VMEM((count // width, width), F32),
            pltpu.VMEM((1, model), F32),
            pltpu.VMEM((ring, count, width), BF16),
            pltpu.VMEM((ring, total, width), BF16),
            pltpu.VMEM((ring_rows, width), BF16),
            pltpu.VMEM((ring, total - ring_rows, width), BF16),
            pltpu.VMEM((model, hidden), BF16),
            pltpu.VMEM((hidden, model), BF16),
            pltpu.VMEM((model, hidden), BF16),
            pltpu.VMEM((hidden, model), BF16),
            pltpu.VMEM((ring, count, width), F32),
            pltpu.VMEM((ring, far_rows, width), F32),
            pltpu.VMEM((2, tiles, messages, res_half, width), BF16),
            pltpu.VMEM((2, tiles, messages, res_half, width), BF16),
            pltpu.VMEM((2, chunks - 1, messages, exp_half, width), BF16),
            pltpu.VMEM((2, chunks - 1, messages, exp_half, width), BF16),
            pltpu.VMEM((far_rows, width), BF16),
            pltpu.VMEM((far_rows, width), BF16),
            pltpu.VMEM((near_rows, model), BF16),
            pltpu.VMEM((near_rows, model), BF16),
            pltpu.VMEM((count, total), BF16),
            pltpu.VMEM((count, width), F32),
            sems((11,)),
            sems((2, gathered)),
            sems((2, gathered)),
            sems((2, gathered)),
            sems((2, gathered)),
            sems((3,)),
            sems((3,)),
            sems((2, tiles, messages)),
            sems((2, tiles, messages)),
            sems((2, chunks - 1, messages)),
            sems((2, chunks - 1, messages)),
            sems((2,)),
            sems((2,)),
        ],
        compiler_params=pltpu.CompilerParams(
            collective_id=0, has_side_effects=True, vmem_limit_bytes=56 * 1024 * 1024
        ),
        name="moe_layer",
    )(
        expert_of.reshape(-1, width), slot_of.reshape(-1, width), gate_prob.reshape(-1, width),
        gain.reshape(1, model), tokens, w_res_in, w_res_out, w_exp_in[0], w_exp_out[0],
    ).astype(BF16)


def solution(mesh):
    return jax.shard_map(
        functools.partial(per_device, mesh.shape["expert"], mesh.shape["mp"]),
        mesh=mesh,
        in_specs=(
            P(("groups", "expert"), "mp"),
            P(),
            P(None, "mp"),
            P("mp", None),
            P("expert", None, "mp"),
            P("expert", "mp", None),
            P(("groups", "expert")),
            P(("groups", "expert")),
            P(("groups", "expert")),
        ),
        out_specs=P(("groups", "expert"), "mp"),
        check_vma=False,
    )
```

```python
import functools

import jax
import jax.numpy as jnp
from jax import lax
from jax.experimental import pallas as pl
from jax.experimental.pallas import tpu as pltpu
from jax.sharding import PartitionSpec as P

MESH = pl.DeviceIdType.MESH
BF16 = jnp.bfloat16
F32 = jnp.float32


def rms_rows(pieces, gain):
    values = jnp.concatenate([piece.astype(F32) for piece in pieces], axis=1)
    inverse = lax.rsqrt(jnp.mean(values * values, axis=-1, keepdims=True) + 1e-05)
    return (values * inverse * gain).astype(BF16)


def mlp_rows(rows, w_in, w_out):
    hidden = jax.nn.gelu(jnp.dot(rows, w_in[...], preferred_element_type=F32)).astype(BF16)
    return jnp.dot(hidden, w_out[...], preferred_element_type=F32)


def remote(src, dst, send_sem, recv_sem, axis, device):
    return pltpu.make_async_remote_copy(
        src_ref=src,
        dst_ref=dst,
        send_sem=send_sem,
        recv_sem=recv_sem,
        device_id={axis: device},
        device_id_type=MESH,
    )


def layer_kernel(
    experts, ring, slots, chunks, tiles, pieces,
    ids_hbm, slots_hbm, gate_hbm, gain_hbm, tok_hbm, wri_hbm, wro_hbm, wei_hbm, weo_hbm, out,
    ids, slot, gate, gain_row, tok_all, exp_all, outgoing, near_out, wri, wro, wei, weo,
    res_part, exp_part, rs_send, rs_recv, es_send, es_recv, ret_send, returned,
    near_ret, near_in, table, gate_cols, result,
    local_sem, out_sem, tok_ss, tok_rs, exp_ss, exp_rs, dis_ss, dis_rs,
    rs_ss, rs_rs, es_ss, es_rs, ret_ss, ret_rs,
):
    me = lax.axis_index("mp")
    mine = lax.axis_index("expert")
    tokens, width = out.shape
    total = experts * slots
    messages = ring - 1
    chunk_rows = total // chunks
    per_chunk = experts // chunks
    near_blocks = per_chunk
    mid_blocks = per_chunk // 2
    far_blocks = experts - near_blocks
    ring_blocks = far_blocks - mid_blocks
    far_rows = far_blocks * slots
    ring_rows = ring_blocks * slots

    def on_ring(offset):
        return lax.rem(me + offset + 2 * ring, ring)

    def partner(p):
        far = lax.div(p + 1, 2)
        return experts // 2 + jnp.where(lax.rem(p, 2) == 0, far, -far)

    def expert_at(p):
        return lax.rem(mine - partner(p) + experts, experts)

    def source_at(p):
        return lax.rem(mine + partner(p), experts)

    def block(at):
        return pl.ds(pl.multiple_of(at * slots, slots), slots)

    def blocks(first, count):
        return pl.ds(first * slots, count * slots)

    tok_copy = pltpu.make_async_copy(tok_hbm, tok_all.at[me], local_sem.at[0])
    tok_copy.start()

    barrier = pltpu.get_barrier_semaphore()
    for offset in (-1, 1):
        pl.semaphore_signal(
            barrier, inc=1, device_id={"mp": on_ring(offset)}, device_id_type=MESH
        )

    def greet(step, carry):
        pl.semaphore_signal(
            barrier,
            inc=1,
            device_id={"expert": lax.rem(mine + step, experts)},
            device_id_type=MESH,
        )
        return carry

    lax.fori_loop(1, experts, greet, 0)

    small_copies = [
        pltpu.make_async_copy(src, dst, local_sem.at[7 + at])
        for at, (src, dst) in enumerate(
            ((ids_hbm, ids), (slots_hbm, slot), (gate_hbm, gate), (gain_hbm, gain_row))
        )
    ]
    for copy in small_copies:
        copy.start()
    weight_copies = [
        pltpu.make_async_copy(src, dst, local_sem.at[1 + at])
        for at, (src, dst) in enumerate(
            ((wri_hbm, wri), (wro_hbm, wro), (wei_hbm, wei), (weo_hbm, weo))
        )
    ]
    for copy in weight_copies:
        copy.start()
    for copy in small_copies:
        copy.wait()
    tok_copy.wait()
    pl.semaphore_wait(barrier, experts + 1)

    gathered = messages * pieces // 2

    def gather_copy(refs, j, way, arriving):
        buf, rows, send_sem, recv_sem = refs
        turn = 1 - 2 * way
        size = rows // pieces
        shard = on_ring(-turn * (j // pieces + (1 if arriving else 0)))
        piece = (j + way * (pieces // 2)) % pieces
        ref = buf.at[shard, pl.ds(piece * size, size)]
        return remote(ref, ref, send_sem.at[way, j], recv_sem.at[way, j], "mp", on_ring(turn))

    def gather_send(refs):
        for j in range(pieces):
            for way in (0, 1):
                gather_copy(refs, j, way, False).start()

    def gather_step(refs, j):
        for way in (0, 1):
            gather_copy(refs, j, way, True).wait_recv()
            if j + pieces < gathered:
                gather_copy(refs, j + pieces, way, False).start()

    tok_ring = (tok_all, tokens, tok_ss, tok_rs)
    exp_ring = (exp_all, ring_rows, exp_ss, exp_rs)
    gather_send(tok_ring)

    def as_row(values):
        return jnp.concatenate([values[at : at + 1] for at in range(values.shape[0])], axis=1)

    slot_row = as_row(jnp.where(slot[...] >= 0, ids[...] * slots + slot[...], -1))

    def send_hits(first, count):
        step = lax.broadcasted_iota(jnp.int32, (slots, tokens), 0)
        hits = [
            jnp.where(step + expert_at(first + at) * slots == slot_row, 1.0, 0.0)
            for at in range(count)
        ]
        return jnp.concatenate(hits, axis=0).astype(BF16)

    def dispatch(p, carry):
        remote(
            outgoing.at[block(p)], exp_all.at[me, block(p)],
            dis_ss.at[0], dis_rs.at[0], "expert", expert_at(p),
        ).start()
        return carry

    group = mid_blocks

    def pick(c, carry):
        rows = pl.ds(pl.multiple_of(c * group * slots, slots), group * slots)
        outgoing[rows, :] = jnp.dot(
            send_hits(c * group, group), tok_all[me], preferred_element_type=F32
        ).astype(BF16)
        return lax.fori_loop(c * group, (c + 1) * group, dispatch, carry)

    lax.fori_loop(0, ring_blocks // group, pick, 0)

    def turned(row):
        return jnp.transpose(jnp.broadcast_to(row, (width, tokens)))

    gate_cols[...] = turned(as_row(gate[...]))
    slot_cols = turned(slot_row.astype(F32))
    lane = lax.broadcasted_iota(jnp.int32, (1, total), 1)
    wanted = jnp.zeros((1, total), jnp.int32)
    for p in range(experts):
        inside = jnp.logical_and(lane >= p * slots, lane < (p + 1) * slots)
        wanted = jnp.where(inside, lane + (expert_at(p) - p) * slots, wanted)
    wanted = wanted.astype(F32)
    for at in range(0, total, width):
        wide = min(width, total - at)
        hit = jnp.where(slot_cols[:, :wide] == wanted[:, at : at + wide], 1.0, 0.0)
        table[:, at : at + wide] = hit.astype(BF16)

    for j in range(gathered - pieces):
        gather_step(tok_ring, j)

    anyone = lax.rem(mine + 1, experts)
    far = blocks(0, far_blocks)
    ringed = blocks(0, ring_blocks)

    def all_dispatched():
        return remote(
            outgoing.at[ringed], exp_all.at[me, ringed], dis_ss.at[0], dis_rs.at[0], "expert", anyone,
        )

    all_dispatched().wait_recv()
    gather_send(exp_ring)
    for j in range(gathered - pieces, gathered):
        gather_step(tok_ring, j)

    def whole_copy(first, count, sem, target):
        return remote(
            near_out.at[:, pl.ds(pl.multiple_of((first - ring_blocks) * slots, slots), count * slots), :],
            exp_all.at[:, pl.ds(pl.multiple_of(first * slots, slots), count * slots), :],
            dis_ss.at[sem], dis_rs.at[sem], "expert", target,
        )

    def dispatch_whole(first, count, last, sem):
        hits = send_hits(first, count)
        rows = pl.ds((first - ring_blocks) * slots, count * slots)
        for k in range(ring):
            near_out[k, rows, :] = jnp.dot(
                hits, tok_all[k], preferred_element_type=F32
            ).astype(BF16)

        def one(p, carry):
            whole_copy(p, 1, sem, expert_at(p)).start()
            return carry

        lax.fori_loop(first, last, one, 0)

    dispatch_whole(far_blocks, near_blocks, experts - 1, 1)
    own_copy = pltpu.make_async_copy(
        near_out.at[:, blocks(experts - 1 - ring_blocks, 1), :],
        exp_all.at[:, blocks(experts - 1, 1), :],
        local_sem.at[5],
    )
    own_copy.start()
    exp_steps = iter(range(gathered))

    def exp_advance(count):
        for j in range(count):
            gather_step(exp_ring, next(exp_steps))

    exp_advance(1)
    dispatch_whole(ring_blocks, mid_blocks, far_blocks, 2)

    def all_near():
        return whole_copy(far_blocks, near_blocks - 1, 1, anyone)

    def all_mid():
        return whole_copy(ring_blocks, mid_blocks, 2, anyone)

    gain = gain_row[...]
    weight_copies[0].wait()
    weight_copies[1].wait()
    res_rows = tokens // tiles
    relayed = gathered - pieces
    for tile in range(tiles):
        exp_advance((relayed - 1) // (tiles + 1))
        rows = pl.ds(tile * res_rows, res_rows)
        normed = rms_rows([tok_all[k, rows, :] for k in range(ring)], gain)
        part = mlp_rows(normed, wri, wro)
        for k in range(ring):
            res_part[k, rows, :] = part[:, k * width : (k + 1) * width]
    exp_advance(relayed - 1 - tiles * ((relayed - 1) // (tiles + 1)))

    def expert_rows(c):
        rows = pl.ds(pl.multiple_of(c * chunk_rows, chunk_rows), chunk_rows)
        normed = rms_rows([exp_all[k, rows, :] for k in range(ring)], gain)
        return rows, mlp_rows(normed, wei, weo)

    weight_copies[2].wait()
    weight_copies[3].wait()
    own_copy.wait()
    all_near().wait_recv()
    near_ret[...] = expert_rows(chunks - 1)[1].astype(BF16)

    def give_near(p, carry):
        remote(
            near_ret.at[block(p - far_blocks)], near_in.at[block(p - far_blocks)],
            ret_ss.at[1], ret_rs.at[1], "expert", source_at(p),
        ).start()
        return carry

    lax.fori_loop(far_blocks, experts - 1, give_near, 0)
    last_block = blocks(per_chunk - 1, 1)
    own_back = pltpu.make_async_copy(
        near_ret.at[last_block], near_in.at[last_block], local_sem.at[6]
    )
    own_back.start()

    def all_near_back():
        others = blocks(0, near_blocks - 1)
        return remote(
            near_ret.at[others], near_in.at[others], ret_ss.at[1], ret_rs.at[1], "expert", anyone,
        )

    exp_advance(pieces)

    def scatter_copy(refs, c, j, way):
        send, recv, send_sem, recv_sem = refs[1:]
        return remote(
            send.at[way, c, j], recv.at[way, c, j],
            send_sem.at[way, c, j], recv_sem.at[way, c, j], "mp", on_ring(1 - 2 * way),
        )

    def scatter_send(refs, c, j):
        part, send, recv = refs[:3]
        half = send.shape[3]
        for way in (0, 1):
            turn = 1 - 2 * way
            dest = on_ring(turn * (ring // 2 - (j + 1) // 2))
            start = pl.multiple_of(c * 2 * half + ((j + way) % 2) * half, half)
            value = part[dest, pl.ds(start, half), :]
            if j >= 2:
                scatter_copy(refs, c, j - 2, way).wait_recv()
                value = value + recv[way, c, j - 2].astype(F32)
            send[way, c, j] = value.astype(BF16)
            scatter_copy(refs, c, j, way).start()

    def scatter_sum(refs, c, h):
        part, send, recv = refs[:3]
        half = send.shape[3]
        start = pl.multiple_of(c * 2 * half + h * half, half)
        value = part[me, pl.ds(start, half), :]
        for way in (0, 1):
            j = messages - 1 if h == way else messages - 2
            scatter_copy(refs, c, j, way).wait_recv()
            value = value + recv[way, c, j].astype(F32)
        return value

    res_sums = (res_part, rs_send, rs_recv, rs_ss, rs_rs)
    exp_sums = (exp_part, es_send, es_recv, es_ss, es_rs)

    def expert(c):
        rows, part = expert_rows(c)
        for k in range(ring):
            exp_part[k, rows, :] = part[:, k * width : (k + 1) * width]

    def merge():
        own_back.wait()
        all_near_back().wait_recv()
        near_rows = pl.ds(far_rows, chunk_rows)
        for tile in range(tiles):
            rows = pl.ds(tile * res_rows, res_rows)
            back = jnp.dot(table[rows, near_rows], near_in[...], preferred_element_type=F32)
            gates = gate_cols[rows, :]
            for k in range(ring):
                res_part[k, rows, :] += gates * back[:, k * width : (k + 1) * width]

    def give_back(p, carry):
        remote(
            ret_send.at[block(p)], returned.at[block(p)],
            ret_ss.at[0], ret_rs.at[0], "expert", source_at(p),
        ).start()
        return carry

    half_rows = chunk_rows // 2

    def finish(c):
        for h in (0, 1):
            ret_send[pl.ds(c * chunk_rows + h * half_rows, half_rows), :] = scatter_sum(
                exp_sums, c, h
            ).astype(BF16)
        lax.fori_loop(c * per_chunk, (c + 1) * per_chunk, give_back, 0)

    def wave(refs, first, last, *steps):
        def one(c, carry, j=0):
            scatter_send(refs, c, j)
            return carry

        for j in steps:
            if j < messages:
                lax.fori_loop(first, last, functools.partial(one, j=j), 0)

    lead = chunks - 2

    def lead_wave(*steps):
        wave(exp_sums, 0, lead, *steps)

    def last_wave(*steps):
        wave(exp_sums, lead, lead + 1, *steps)

    def res_wave(*steps):
        wave(res_sums, 0, tiles, *steps)

    for c in range(lead):
        expert(c)
        scatter_send(exp_sums, c, 0)
        scatter_send(exp_sums, c, 1)
    lead_wave(2)
    all_mid().wait_recv()
    expert(lead)
    last_wave(0, 1)
    lead_wave(3, 4)
    last_wave(2)
    merge()
    res_wave(0)
    lead_wave(5)
    last_wave(3)
    lead_wave(6)
    last_wave(4)
    res_wave(1)
    for c in range(lead):
        finish(c)
    res_wave(2)
    last_wave(5)
    res_wave(3)
    last_wave(6)
    res_wave(4)
    finish(lead)
    res_wave(5, 6)

    def all_returned():
        return remote(
            ret_send.at[far], returned.at[far], ret_ss.at[0], ret_rs.at[0], "expert", anyone,
        )

    all_returned().wait_recv()
    half = res_rows // 2
    parts = [pl.ds(at * half, half) for at in range(2 * tiles)]
    gated = [
        gate_cols[rows, :]
        * jnp.dot(table[rows, pl.ds(0, far_rows)], returned[...], preferred_element_type=F32)
        for rows in parts
    ]
    writes = []
    for at, rows in enumerate(parts):
        value = scatter_sum(res_sums, at // 2, at % 2) + gated[at]
        result[rows, :] = value.astype(BF16)
        writes.append(pltpu.make_async_copy(result.at[rows], out.at[rows], out_sem.at[at]))
        writes[at].start()

    all_dispatched().wait_send()
    all_near().wait_send()
    all_mid().wait_send()
    all_near_back().wait_send()
    all_returned().wait_send()
    for j in range(gathered):
        for way in (0, 1):
            gather_copy(tok_ring, j, way, False).wait_send()
            gather_copy(exp_ring, j, way, False).wait_send()

    def drain(refs, c, carry):
        for j in range(messages):
            for way in (0, 1):
                scatter_copy(refs, c, j, way).wait_send()
        return carry

    lax.fori_loop(0, tiles, functools.partial(drain, res_sums), 0)
    lax.fori_loop(0, chunks - 1, functools.partial(drain, exp_sums), 0)
    for write in writes:
        write.wait()


def per_device(
    experts, ring, tokens, gain, w_res_in, w_res_out, w_exp_in, w_exp_out,
    expert_of, slot_of, gate_prob,
):
    count, width = tokens.shape
    model, hidden = w_res_in.shape
    capacity = max(2, 5 * count // (4 * experts))
    slots = -(-capacity // 16) * 16
    chunks = 4 if experts % 8 == 0 else 2
    total = experts * slots
    messages = ring - 1
    near_rows = total // chunks
    far_rows = total - near_rows
    ring_rows = far_rows - near_rows // 2

    any_space = pl.BlockSpec(memory_space=pl.ANY)
    sems = pltpu.SemaphoreType.DMA
    tiles = 3 if count % 96 == 0 else 1
    pieces = 4
    gathered = messages * pieces // 2
    res_half, exp_half = count // tiles // 2, total // chunks // 2
    return pl.pallas_call(
        functools.partial(layer_kernel, experts, ring, slots, chunks, tiles, pieces),
        out_shape=jax.ShapeDtypeStruct((count, width), BF16),
        in_specs=[any_space] * 9,
        out_specs=any_space,
        scratch_shapes=[
            pltpu.VMEM((count // width, width), jnp.int32),
            pltpu.VMEM((count // width, width), jnp.int32),
            pltpu.VMEM((count // width, width), F32),
            pltpu.VMEM((1, model), F32),
            pltpu.VMEM((ring, count, width), BF16),
            pltpu.VMEM((ring, total, width), BF16),
            pltpu.VMEM((ring_rows, width), BF16),
            pltpu.VMEM((ring, total - ring_rows, width), BF16),
            pltpu.VMEM((model, hidden), BF16),
            pltpu.VMEM((hidden, model), BF16),
            pltpu.VMEM((model, hidden), BF16),
            pltpu.VMEM((hidden, model), BF16),
            pltpu.VMEM((ring, count, width), F32),
            pltpu.VMEM((ring, far_rows, width), F32),
            pltpu.VMEM((2, tiles, messages, res_half, width), BF16),
            pltpu.VMEM((2, tiles, messages, res_half, width), BF16),
            pltpu.VMEM((2, chunks - 1, messages, exp_half, width), BF16),
            pltpu.VMEM((2, chunks - 1, messages, exp_half, width), BF16),
            pltpu.VMEM((far_rows, width), BF16),
            pltpu.VMEM((far_rows, width), BF16),
            pltpu.VMEM((near_rows, model), BF16),
            pltpu.VMEM((near_rows, model), BF16),
            pltpu.VMEM((count, total), BF16),
            pltpu.VMEM((count, width), F32),
            pltpu.VMEM((count, width), BF16),
            sems((11,)),
            sems((2 * tiles,)),
            sems((2, gathered)),
            sems((2, gathered)),
            sems((2, gathered)),
            sems((2, gathered)),
            sems((3,)),
            sems((3,)),
            sems((2, tiles, messages)),
            sems((2, tiles, messages)),
            sems((2, chunks - 1, messages)),
            sems((2, chunks - 1, messages)),
            sems((2,)),
            sems((2,)),
        ],
        compiler_params=pltpu.CompilerParams(
            collective_id=0, has_side_effects=True, vmem_limit_bytes=56 * 1024 * 1024
        ),
        name="moe_layer",
    )(
        expert_of.reshape(-1, width), slot_of.reshape(-1, width), gate_prob.reshape(-1, width),
        gain.reshape(1, model), tokens, w_res_in, w_res_out, w_exp_in[0], w_exp_out[0],
    )


def solution(mesh):
    return jax.shard_map(
        functools.partial(per_device, mesh.shape["expert"], mesh.shape["mp"]),
        mesh=mesh,
        in_specs=(
            P(("groups", "expert"), "mp"),
            P(),
            P(None, "mp"),
            P("mp", None),
            P("expert", None, "mp"),
            P("expert", "mp", None),
            P(("groups", "expert")),
            P(("groups", "expert")),
            P(("groups", "expert")),
        ),
        out_specs=P(("groups", "expert"), "mp"),
        check_vma=False,
    )
```

```python
import functools

import jax
import jax.numpy as jnp
from jax import lax
from jax.experimental import pallas as pl
from jax.experimental.pallas import tpu as pltpu
from jax.sharding import PartitionSpec as P

MESH = pl.DeviceIdType.MESH
BF16 = jnp.bfloat16
F32 = jnp.float32


def rms_rows(pieces, gain):
    values = jnp.concatenate([piece.astype(F32) for piece in pieces], axis=1)
    inverse = lax.rsqrt(jnp.mean(values * values, axis=-1, keepdims=True) + 1e-05)
    return (values * inverse * gain).astype(BF16)


def mlp_rows(rows, w_in, w_out):
    hidden = jax.nn.gelu(jnp.dot(rows, w_in[...], preferred_element_type=F32)).astype(BF16)
    return jnp.dot(hidden, w_out[...], preferred_element_type=F32)


def remote(src, dst, send_sem, recv_sem, axis, device):
    return pltpu.make_async_remote_copy(
        src_ref=src,
        dst_ref=dst,
        send_sem=send_sem,
        recv_sem=recv_sem,
        device_id={axis: device},
        device_id_type=MESH,
    )


def layer_kernel(
    experts, ring, slots, chunks, tiles, pieces,
    ids_hbm, slots_hbm, gate_hbm, gain_hbm, tok_hbm, wri_hbm, wro_hbm, wei_hbm, weo_hbm, out,
    ids, slot, gate, gain_row, tok_all, exp_all, outgoing, near_out, wri, wro, wei, weo,
    res_part, exp_part, rs_send, rs_recv, es_send, es_recv, ret_send, returned,
    near_ret, near_in, table, gate_cols,
    local_sem, tok_ss, tok_rs, exp_ss, exp_rs, dis_ss, dis_rs,
    rs_ss, rs_rs, es_ss, es_rs, ret_ss, ret_rs,
):
    me = lax.axis_index("mp")
    mine = lax.axis_index("expert")
    tokens, width = out.shape
    total = experts * slots
    messages = ring - 1
    chunk_rows = total // chunks
    per_chunk = experts // chunks
    near_blocks = per_chunk
    mid_blocks = per_chunk // 4 or 1
    far_blocks = experts - near_blocks
    ring_blocks = far_blocks - mid_blocks
    far_rows = far_blocks * slots
    ring_rows = ring_blocks * slots

    def on_ring(offset):
        return lax.rem(me + offset + 2 * ring, ring)

    def partner(p):
        far = lax.div(p + 1, 2)
        return experts // 2 + jnp.where(lax.rem(p, 2) == 0, far, -far)

    def expert_at(p):
        return lax.rem(mine - partner(p) + experts, experts)

    def source_at(p):
        return lax.rem(mine + partner(p), experts)

    def block(at):
        return pl.ds(pl.multiple_of(at * slots, slots), slots)

    def blocks(first, count):
        return pl.ds(first * slots, count * slots)

    tok_copy = pltpu.make_async_copy(tok_hbm, tok_all.at[me], local_sem.at[0])
    tok_copy.start()

    barrier = pltpu.get_barrier_semaphore()
    for offset in (-1, 1):
        pl.semaphore_signal(
            barrier, inc=1, device_id={"mp": on_ring(offset)}, device_id_type=MESH
        )

    def greet(step, carry):
        pl.semaphore_signal(
            barrier,
            inc=1,
            device_id={"expert": lax.rem(mine + step, experts)},
            device_id_type=MESH,
        )
        return carry

    lax.fori_loop(1, experts, greet, 0)

    small_copies = [
        pltpu.make_async_copy(src, dst, local_sem.at[7 + at])
        for at, (src, dst) in enumerate(
            ((ids_hbm, ids), (slots_hbm, slot), (gate_hbm, gate), (gain_hbm, gain_row))
        )
    ]
    for copy in small_copies:
        copy.start()
    weight_copies = [
        pltpu.make_async_copy(src, dst, local_sem.at[1 + at])
        for at, (src, dst) in enumerate(
            ((wri_hbm, wri), (wro_hbm, wro), (wei_hbm, wei), (weo_hbm, weo))
        )
    ]
    for copy in weight_copies:
        copy.start()
    for copy in small_copies:
        copy.wait()
    tok_copy.wait()
    pl.semaphore_wait(barrier, experts + 1)

    gathered = messages * pieces // 2

    def gather_copy(refs, j, way, arriving):
        buf, rows, send_sem, recv_sem = refs
        turn = 1 - 2 * way
        size = rows // pieces
        shard = on_ring(-turn * (j // pieces + (1 if arriving else 0)))
        piece = (j + way * (pieces // 2)) % pieces
        ref = buf.at[shard, pl.ds(piece * size, size)]
        return remote(ref, ref, send_sem.at[way, j], recv_sem.at[way, j], "mp", on_ring(turn))

    def gather_send(refs):
        for j in range(pieces):
            for way in (0, 1):
                gather_copy(refs, j, way, False).start()

    def gather_step(refs, j):
        for way in (0, 1):
            gather_copy(refs, j, way, True).wait_recv()
            if j + pieces < gathered:
                gather_copy(refs, j + pieces, way, False).start()

    tok_ring = (tok_all, tokens, tok_ss, tok_rs)
    exp_ring = (exp_all, ring_rows, exp_ss, exp_rs)
    gather_send(tok_ring)

    def as_row(values):
        return jnp.concatenate([values[at : at + 1] for at in range(values.shape[0])], axis=1)

    slot_row = as_row(jnp.where(slot[...] >= 0, ids[...] * slots + slot[...], -1))

    def send_hits(first, count):
        step = lax.broadcasted_iota(jnp.int32, (slots, tokens), 0)
        hits = [
            jnp.where(step + expert_at(first + at) * slots == slot_row, 1.0, 0.0)
            for at in range(count)
        ]
        return jnp.concatenate(hits, axis=0).astype(BF16)

    def dispatch(p, carry):
        remote(
            outgoing.at[block(p)], exp_all.at[me, block(p)],
            dis_ss.at[0], dis_rs.at[0], "expert", expert_at(p),
        ).start()
        return carry

    group = ring_blocks // 2 if ring_blocks % 2 == 0 else ring_blocks

    def pick(c, carry):
        rows = pl.ds(pl.multiple_of(c * group * slots, slots), group * slots)
        outgoing[rows, :] = jnp.dot(
            send_hits(c * group, group), tok_all[me], preferred_element_type=F32
        ).astype(BF16)
        return lax.fori_loop(c * group, (c + 1) * group, dispatch, carry)

    lax.fori_loop(0, ring_blocks // group, pick, 0)

    def turned(row):
        return jnp.transpose(jnp.broadcast_to(row, (width, tokens)))

    gate_cols[...] = turned(as_row(gate[...]))
    slot_cols = turned(slot_row.astype(F32))
    lane = lax.broadcasted_iota(jnp.int32, (1, total), 1)
    wanted = jnp.zeros((1, total), jnp.int32)
    for p in range(experts):
        inside = jnp.logical_and(lane >= p * slots, lane < (p + 1) * slots)
        wanted = jnp.where(inside, lane + (expert_at(p) - p) * slots, wanted)
    wanted = wanted.astype(F32)
    for at in range(0, total, width):
        wide = min(width, total - at)
        hit = jnp.where(slot_cols[:, :wide] == wanted[:, at : at + wide], 1.0, 0.0)
        table[:, at : at + wide] = hit.astype(BF16)

    for j in range(gathered - pieces):
        gather_step(tok_ring, j)

    anyone = lax.rem(mine + 1, experts)
    far = blocks(0, far_blocks)
    ringed = blocks(0, ring_blocks)

    def all_dispatched():
        return remote(
            outgoing.at[ringed], exp_all.at[me, ringed], dis_ss.at[0], dis_rs.at[0], "expert", anyone,
        )

    all_dispatched().wait_recv()
    gather_send(exp_ring)
    for j in range(gathered - pieces, gathered):
        gather_step(tok_ring, j)

    def whole_copy(first, count, sem, target):
        return remote(
            near_out.at[:, pl.ds(pl.multiple_of((first - ring_blocks) * slots, slots), count * slots), :],
            exp_all.at[:, pl.ds(pl.multiple_of(first * slots, slots), count * slots), :],
            dis_ss.at[sem], dis_rs.at[sem], "expert", target,
        )

    def dispatch_whole(first, count, last, sem):
        hits = send_hits(first, count)
        rows = pl.ds((first - ring_blocks) * slots, count * slots)
        for k in range(ring):
            near_out[k, rows, :] = jnp.dot(
                hits, tok_all[k], preferred_element_type=F32
            ).astype(BF16)

        def one(p, carry):
            whole_copy(p, 1, sem, expert_at(p)).start()
            return carry

        lax.fori_loop(first, last, one, 0)

    dispatch_whole(far_blocks, near_blocks, experts - 1, 1)
    own_copy = pltpu.make_async_copy(
        near_out.at[:, blocks(experts - 1 - ring_blocks, 1), :],
        exp_all.at[:, blocks(experts - 1, 1), :],
        local_sem.at[5],
    )
    own_copy.start()
    exp_steps = iter(range(gathered))

    def exp_advance(count):
        for j in range(count):
            gather_step(exp_ring, next(exp_steps))

    exp_advance(1)
    dispatch_whole(ring_blocks, mid_blocks, far_blocks, 2)

    def all_near():
        return whole_copy(far_blocks, near_blocks - 1, 1, anyone)

    def all_mid():
        return whole_copy(ring_blocks, mid_blocks, 2, anyone)

    gain = gain_row[...]
    weight_copies[0].wait()
    weight_copies[1].wait()
    res_rows = tokens // tiles
    relayed = gathered - pieces
    for tile in range(tiles):
        exp_advance((relayed - 1) // (tiles + 1))
        rows = pl.ds(tile * res_rows, res_rows)
        normed = rms_rows([tok_all[k, rows, :] for k in range(ring)], gain)
        part = mlp_rows(normed, wri, wro)
        for k in range(ring):
            res_part[k, rows, :] = part[:, k * width : (k + 1) * width]
    exp_advance(relayed - 1 - tiles * ((relayed - 1) // (tiles + 1)))

    def expert_rows(c):
        rows = pl.ds(pl.multiple_of(c * chunk_rows, chunk_rows), chunk_rows)
        normed = rms_rows([exp_all[k, rows, :] for k in range(ring)], gain)
        return rows, mlp_rows(normed, wei, weo)

    weight_copies[2].wait()
    weight_copies[3].wait()
    own_copy.wait()
    all_near().wait_recv()
    near_ret[...] = expert_rows(chunks - 1)[1].astype(BF16)

    def give_near(p, carry):
        remote(
            near_ret.at[block(p - far_blocks)], near_in.at[block(p - far_blocks)],
            ret_ss.at[1], ret_rs.at[1], "expert", source_at(p),
        ).start()
        return carry

    lax.fori_loop(far_blocks, experts - 1, give_near, 0)
    last_block = blocks(per_chunk - 1, 1)
    own_back = pltpu.make_async_copy(
        near_ret.at[last_block], near_in.at[last_block], local_sem.at[6]
    )
    own_back.start()

    def all_near_back():
        others = blocks(0, near_blocks - 1)
        return remote(
            near_ret.at[others], near_in.at[others], ret_ss.at[1], ret_rs.at[1], "expert", anyone,
        )

    exp_advance(pieces)

    def scatter_copy(refs, c, j, way):
        send, recv, send_sem, recv_sem = refs[1:]
        return remote(
            send.at[way, c, j], recv.at[way, c, j],
            send_sem.at[way, c, j], recv_sem.at[way, c, j], "mp", on_ring(1 - 2 * way),
        )

    def scatter_send(refs, c, j):
        part, send, recv = refs[:3]
        half = send.shape[3]
        for way in (0, 1):
            turn = 1 - 2 * way
            dest = on_ring(turn * (ring // 2 - (j + 1) // 2))
            start = pl.multiple_of(c * 2 * half + ((j + way) % 2) * half, half)
            value = part[dest, pl.ds(start, half), :]
            if j >= 2:
                scatter_copy(refs, c, j - 2, way).wait_recv()
                value = value + recv[way, c, j - 2].astype(F32)
            send[way, c, j] = value.astype(BF16)
            scatter_copy(refs, c, j, way).start()

    def scatter_sum(refs, c, h):
        part, send, recv = refs[:3]
        half = send.shape[3]
        start = pl.multiple_of(c * 2 * half + h * half, half)
        value = part[me, pl.ds(start, half), :]
        for way in (0, 1):
            j = messages - 1 if h == way else messages - 2
            scatter_copy(refs, c, j, way).wait_recv()
            value = value + recv[way, c, j].astype(F32)
        return value

    res_sums = (res_part, rs_send, rs_recv, rs_ss, rs_rs)
    exp_sums = (exp_part, es_send, es_recv, es_ss, es_rs)

    def expert(c):
        rows, part = expert_rows(c)
        for k in range(ring):
            exp_part[k, rows, :] = part[:, k * width : (k + 1) * width]

    def merge():
        own_back.wait()
        all_near_back().wait_recv()
        near_rows = pl.ds(far_rows, chunk_rows)
        for tile in range(tiles):
            rows = pl.ds(tile * res_rows, res_rows)
            back = jnp.dot(table[rows, near_rows], near_in[...], preferred_element_type=F32)
            gates = gate_cols[rows, :]
            for k in range(ring):
                res_part[k, rows, :] += gates * back[:, k * width : (k + 1) * width]

    def give_back(p, carry):
        remote(
            ret_send.at[block(p)], returned.at[block(p)],
            ret_ss.at[0], ret_rs.at[0], "expert", source_at(p),
        ).start()
        return carry

    half_rows = chunk_rows // 2

    def finish(c):
        for h in (0, 1):
            ret_send[pl.ds(c * chunk_rows + h * half_rows, half_rows), :] = scatter_sum(
                exp_sums, c, h
            ).astype(BF16)
        lax.fori_loop(c * per_chunk, (c + 1) * per_chunk, give_back, 0)

    def wave(refs, first, last, *steps):
        def one(c, carry, j=0):
            scatter_send(refs, c, j)
            return carry

        for j in steps:
            if j < messages:
                lax.fori_loop(first, last, functools.partial(one, j=j), 0)

    lead = chunks - 2

    def lead_wave(*steps):
        wave(exp_sums, 0, lead, *steps)

    def last_wave(*steps):
        wave(exp_sums, lead, lead + 1, *steps)

    def res_wave(*steps):
        wave(res_sums, 0, tiles, *steps)

    for c in range(lead):
        expert(c)
        scatter_send(exp_sums, c, 0)
        scatter_send(exp_sums, c, 1)
    all_mid().wait_recv()
    expert(lead)
    last_wave(0, 1)
    lead_wave(2)
    last_wave(2)
    lead_wave(3)
    merge()
    res_wave(0)
    lead_wave(4)
    last_wave(3)
    lead_wave(5)
    res_wave(1)
    lead_wave(6)
    last_wave(4)
    for c in range(lead):
        finish(c)
    last_wave(5)
    res_wave(2)
    last_wave(6)
    res_wave(3)
    finish(lead)
    res_wave(4, 5, 6)

    def all_returned():
        return remote(
            ret_send.at[far], returned.at[far], ret_ss.at[0], ret_rs.at[0], "expert", anyone,
        )

    all_returned().wait_recv()
    half = res_rows // 2
    parts = [pl.ds(at * half, half) for at in range(2 * tiles)]
    gated = [
        gate_cols[rows, :]
        * jnp.dot(table[rows, pl.ds(0, far_rows)], returned[...], preferred_element_type=F32)
        for rows in parts
    ]
    for at, rows in enumerate(parts):
        value = scatter_sum(res_sums, at // 2, at % 2) + gated[at]
        out[rows, :] = value.astype(BF16)

    all_dispatched().wait_send()
    all_near().wait_send()
    all_mid().wait_send()
    all_near_back().wait_send()
    all_returned().wait_send()
    for j in range(gathered):
        for way in (0, 1):
            gather_copy(tok_ring, j, way, False).wait_send()
            gather_copy(exp_ring, j, way, False).wait_send()

    def drain(refs, c, carry):
        for j in range(messages):
            for way in (0, 1):
                scatter_copy(refs, c, j, way).wait_send()
        return carry

    lax.fori_loop(0, tiles, functools.partial(drain, res_sums), 0)
    lax.fori_loop(0, chunks - 1, functools.partial(drain, exp_sums), 0)


def per_device(
    experts, ring, tokens, gain, w_res_in, w_res_out, w_exp_in, w_exp_out,
    expert_of, slot_of, gate_prob,
):
    count, width = tokens.shape
    model, hidden = w_res_in.shape
    capacity = max(2, 5 * count // (4 * experts))
    slots = -(-capacity // 16) * 16
    chunks = 4 if experts % 8 == 0 else 2
    total = experts * slots
    messages = ring - 1
    near_rows = total // chunks
    far_rows = total - near_rows
    ring_rows = far_rows - (experts // chunks // 4 or 1) * slots

    any_space = pl.BlockSpec(memory_space=pl.ANY)
    sems = pltpu.SemaphoreType.DMA
    tiles = 3 if count % 96 == 0 else 1
    pieces = 4
    gathered = messages * pieces // 2
    res_half, exp_half = count // tiles // 2, total // chunks // 2
    return pl.pallas_call(
        functools.partial(layer_kernel, experts, ring, slots, chunks, tiles, pieces),
        out_shape=pltpu.VMEM((count, width), BF16),
        in_specs=[any_space] * 9,
        out_specs=pl.BlockSpec(memory_space=pltpu.VMEM),
        scratch_shapes=[
            pltpu.VMEM((count // width, width), jnp.int32),
            pltpu.VMEM((count // width, width), jnp.int32),
            pltpu.VMEM((count // width, width), F32),
            pltpu.VMEM((1, model), F32),
            pltpu.VMEM((ring, count, width), BF16),
            pltpu.VMEM((ring, total, width), BF16),
            pltpu.VMEM((ring_rows, width), BF16),
            pltpu.VMEM((ring, total - ring_rows, width), BF16),
            pltpu.VMEM((model, hidden), BF16),
            pltpu.VMEM((hidden, model), BF16),
            pltpu.VMEM((model, hidden), BF16),
            pltpu.VMEM((hidden, model), BF16),
            pltpu.VMEM((ring, count, width), F32),
            pltpu.VMEM((ring, far_rows, width), F32),
            pltpu.VMEM((2, tiles, messages, res_half, width), BF16),
            pltpu.VMEM((2, tiles, messages, res_half, width), BF16),
            pltpu.VMEM((2, chunks - 1, messages, exp_half, width), BF16),
            pltpu.VMEM((2, chunks - 1, messages, exp_half, width), BF16),
            pltpu.VMEM((far_rows, width), BF16),
            pltpu.VMEM((far_rows, width), BF16),
            pltpu.VMEM((near_rows, model), BF16),
            pltpu.VMEM((near_rows, model), BF16),
            pltpu.VMEM((count, total), BF16),
            pltpu.VMEM((count, width), F32),
            sems((11,)),
            sems((2, gathered)),
            sems((2, gathered)),
            sems((2, gathered)),
            sems((2, gathered)),
            sems((3,)),
            sems((3,)),
            sems((2, tiles, messages)),
            sems((2, tiles, messages)),
            sems((2, chunks - 1, messages)),
            sems((2, chunks - 1, messages)),
            sems((2,)),
            sems((2,)),
        ],
        compiler_params=pltpu.CompilerParams(
            collective_id=0, has_side_effects=True, vmem_limit_bytes=56 * 1024 * 1024
        ),
        name="moe_layer",
    )(
        expert_of.reshape(-1, width), slot_of.reshape(-1, width), gate_prob.reshape(-1, width),
        gain.reshape(1, model), tokens, w_res_in, w_res_out, w_exp_in[0], w_exp_out[0],
    )


def solution(mesh):
    return jax.shard_map(
        functools.partial(per_device, mesh.shape["expert"], mesh.shape["mp"]),
        mesh=mesh,
        in_specs=(
            P(("groups", "expert"), "mp"),
            P(),
            P(None, "mp"),
            P("mp", None),
            P("expert", None, "mp"),
            P("expert", "mp", None),
            P(("groups", "expert")),
            P(("groups", "expert")),
            P(("groups", "expert")),
        ),
        out_specs=P(("groups", "expert"), "mp"),
        check_vma=False,
    )
```

```python
import functools

import jax
import jax.numpy as jnp
from jax import lax
from jax.experimental import pallas as pl
from jax.experimental.pallas import tpu as pltpu
from jax.sharding import PartitionSpec as P

MESH = pl.DeviceIdType.MESH
BF16 = jnp.bfloat16
F32 = jnp.float32


def rms_rows(pieces, gain):
    values = jnp.concatenate([piece.astype(F32) for piece in pieces], axis=1)
    inverse = lax.rsqrt(jnp.mean(values * values, axis=-1, keepdims=True) + 1e-05)
    return (values * inverse * gain).astype(BF16)


def mlp_rows(rows, w_in, w_out):
    hidden = jax.nn.gelu(jnp.dot(rows, w_in[...], preferred_element_type=F32)).astype(BF16)
    return jnp.dot(hidden, w_out[...], preferred_element_type=F32)


def remote(src, dst, send_sem, recv_sem, axis, device):
    return pltpu.make_async_remote_copy(
        src_ref=src,
        dst_ref=dst,
        send_sem=send_sem,
        recv_sem=recv_sem,
        device_id={axis: device},
        device_id_type=MESH,
    )


def layer_kernel(
    experts, ring, slots, chunks, tiles, tok_pieces, pieces,
    ids_hbm, slots_hbm, gate_hbm, gain_hbm, tok_hbm, wri_hbm, wro_hbm, wei_hbm, weo_hbm, out,
    ids, slot, gate, gain_row, tok_all, exp_all, outgoing, near_out, wri, wro, wei, weo,
    res_part, exp_part, rs_send, rs_recv, es_send, es_recv, ret_send, returned,
    near_ret, near_in, table, gate_cols,
    local_sem, tok_ss, tok_rs, exp_ss, exp_rs, dis_ss, dis_rs,
    rs_ss, rs_rs, es_ss, es_rs, ret_ss, ret_rs,
):
    me = lax.axis_index("mp")
    mine = lax.axis_index("expert")
    tokens, width = out.shape
    total = experts * slots
    messages = ring - 1
    chunk_rows = total // chunks
    per_chunk = experts // chunks
    near_blocks = per_chunk
    mid_blocks = per_chunk // 4 or 1
    far_blocks = experts - near_blocks
    ring_blocks = far_blocks - mid_blocks
    far_rows = far_blocks * slots
    ring_rows = ring_blocks * slots

    def on_ring(offset):
        return lax.rem(me + offset + 2 * ring, ring)

    def partner(p):
        far = lax.div(p + 1, 2)
        return experts // 2 + jnp.where(lax.rem(p, 2) == 0, far, -far)

    def expert_at(p):
        return lax.rem(mine - partner(p) + experts, experts)

    def source_at(p):
        return lax.rem(mine + partner(p), experts)

    def block(at):
        return pl.ds(pl.multiple_of(at * slots, slots), slots)

    def blocks(first, count):
        return pl.ds(first * slots, count * slots)

    tok_copy = pltpu.make_async_copy(tok_hbm, tok_all.at[me], local_sem.at[0])
    tok_copy.start()

    barrier = pltpu.get_barrier_semaphore()
    for offset in (-1, 1):
        pl.semaphore_signal(
            barrier, inc=1, device_id={"mp": on_ring(offset)}, device_id_type=MESH
        )

    def greet(step, carry):
        pl.semaphore_signal(
            barrier,
            inc=1,
            device_id={"expert": lax.rem(mine + step, experts)},
            device_id_type=MESH,
        )
        return carry

    lax.fori_loop(1, experts, greet, 0)

    small_copies = [
        pltpu.make_async_copy(src, dst, local_sem.at[7 + at])
        for at, (src, dst) in enumerate(
            ((ids_hbm, ids), (slots_hbm, slot), (gate_hbm, gate), (gain_hbm, gain_row))
        )
    ]
    for copy in small_copies:
        copy.start()
    weight_copies = [
        pltpu.make_async_copy(src, dst, local_sem.at[1 + at])
        for at, (src, dst) in enumerate(
            ((wri_hbm, wri), (wro_hbm, wro), (wei_hbm, wei), (weo_hbm, weo))
        )
    ]
    for copy in weight_copies:
        copy.start()
    tok_copy.wait()
    pl.semaphore_wait(barrier, experts + 1)

    def gather_copy(refs, j, way, arriving):
        buf, rows, pieces, send_sem, recv_sem = refs
        turn = 1 - 2 * way
        size = rows // pieces
        shard = on_ring(-turn * (j // pieces + (1 if arriving else 0)))
        piece = (j + way * (pieces // 2)) % pieces
        ref = buf.at[shard, pl.ds(piece * size, size)]
        return remote(ref, ref, send_sem.at[way, j], recv_sem.at[way, j], "mp", on_ring(turn))

    def gather_send(refs):
        for j in range(refs[2]):
            for way in (0, 1):
                gather_copy(refs, j, way, False).start()

    def gather_step(refs, j):
        for way in (0, 1):
            gather_copy(refs, j, way, True).wait_recv()
            if j + refs[2] < messages * refs[2] // 2:
                gather_copy(refs, j + refs[2], way, False).start()

    tok_ring = (tok_all, tokens, tok_pieces, tok_ss, tok_rs)
    exp_ring = (exp_all, ring_rows, pieces, exp_ss, exp_rs)
    tok_gathered = messages * tok_pieces // 2
    gathered = messages * pieces // 2
    gather_send(tok_ring)
    for copy in small_copies:
        copy.wait()

    def as_row(values):
        return jnp.concatenate([values[at : at + 1] for at in range(values.shape[0])], axis=1)

    slot_row = as_row(jnp.where(slot[...] >= 0, ids[...] * slots + slot[...], -1))

    def send_hits(first, count):
        step = lax.broadcasted_iota(jnp.int32, (slots, tokens), 0)
        hits = [
            jnp.where(step + expert_at(first + at) * slots == slot_row, 1.0, 0.0)
            for at in range(count)
        ]
        return jnp.concatenate(hits, axis=0).astype(BF16)

    def dispatch(p, carry):
        remote(
            outgoing.at[block(p)], exp_all.at[me, block(p)],
            dis_ss.at[0], dis_rs.at[0], "expert", expert_at(p),
        ).start()
        return carry

    group = ring_blocks // 2 if ring_blocks % 2 == 0 else ring_blocks

    def pick(c, carry):
        rows = pl.ds(pl.multiple_of(c * group * slots, slots), group * slots)
        outgoing[rows, :] = jnp.dot(
            send_hits(c * group, group), tok_all[me], preferred_element_type=F32
        ).astype(BF16)
        return lax.fori_loop(c * group, (c + 1) * group, dispatch, carry)

    lax.fori_loop(0, ring_blocks // group, pick, 0)

    def turned(row):
        return jnp.transpose(jnp.broadcast_to(row, (width, tokens)))

    gate_cols[...] = turned(as_row(gate[...]))
    slot_cols = turned(slot_row.astype(F32))
    lane = lax.broadcasted_iota(jnp.int32, (1, total), 1)
    wanted = jnp.zeros((1, total), jnp.int32)
    for p in range(experts):
        inside = jnp.logical_and(lane >= p * slots, lane < (p + 1) * slots)
        wanted = jnp.where(inside, lane + (expert_at(p) - p) * slots, wanted)
    wanted = wanted.astype(F32)
    for at in range(0, total, width):
        wide = min(width, total - at)
        hit = jnp.where(slot_cols[:, :wide] == wanted[:, at : at + wide], 1.0, 0.0)
        table[:, at : at + wide] = hit.astype(BF16)

    for j in range(tok_gathered - tok_pieces):
        gather_step(tok_ring, j)

    anyone = lax.rem(mine + 1, experts)
    far = blocks(0, far_blocks)
    ringed = blocks(0, ring_blocks)

    def all_dispatched():
        return remote(
            outgoing.at[ringed], exp_all.at[me, ringed], dis_ss.at[0], dis_rs.at[0], "expert", anyone,
        )

    all_dispatched().wait_recv()
    gather_send(exp_ring)
    for j in range(tok_gathered - tok_pieces, tok_gathered):
        gather_step(tok_ring, j)

    def whole_copy(first, count, sem, target):
        return remote(
            near_out.at[:, pl.ds(pl.multiple_of((first - ring_blocks) * slots, slots), count * slots), :],
            exp_all.at[:, pl.ds(pl.multiple_of(first * slots, slots), count * slots), :],
            dis_ss.at[sem], dis_rs.at[sem], "expert", target,
        )

    def dispatch_whole(first, count, last, sem):
        hits = send_hits(first, count)
        rows = pl.ds((first - ring_blocks) * slots, count * slots)
        for k in range(ring):
            near_out[k, rows, :] = jnp.dot(
                hits, tok_all[k], preferred_element_type=F32
            ).astype(BF16)

        def one(p, carry):
            whole_copy(p, 1, sem, expert_at(p)).start()
            return carry

        lax.fori_loop(first, last, one, 0)

    dispatch_whole(far_blocks, near_blocks, experts - 1, 1)
    own_copy = pltpu.make_async_copy(
        near_out.at[:, blocks(experts - 1 - ring_blocks, 1), :],
        exp_all.at[:, blocks(experts - 1, 1), :],
        local_sem.at[5],
    )
    own_copy.start()
    exp_steps = iter(range(gathered))

    def exp_advance(count):
        for j in range(count):
            gather_step(exp_ring, next(exp_steps))

    exp_advance(1)
    dispatch_whole(ring_blocks, mid_blocks, far_blocks, 2)

    def all_near():
        return whole_copy(far_blocks, near_blocks - 1, 1, anyone)

    def all_mid():
        return whole_copy(ring_blocks, mid_blocks, 2, anyone)

    gain = gain_row[...]
    weight_copies[0].wait()
    weight_copies[1].wait()
    res_rows = tokens // tiles
    relayed = gathered - pieces
    for tile in range(tiles):
        exp_advance((relayed - 1) // (tiles + 1))
        rows = pl.ds(tile * res_rows, res_rows)
        normed = rms_rows([tok_all[k, rows, :] for k in range(ring)], gain)
        part = mlp_rows(normed, wri, wro)
        for k in range(ring):
            res_part[k, rows, :] = part[:, k * width : (k + 1) * width]
    exp_advance(relayed - 1 - tiles * ((relayed - 1) // (tiles + 1)))

    def expert_rows(c):
        rows = pl.ds(pl.multiple_of(c * chunk_rows, chunk_rows), chunk_rows)
        normed = rms_rows([exp_all[k, rows, :] for k in range(ring)], gain)
        return rows, mlp_rows(normed, wei, weo)

    weight_copies[2].wait()
    weight_copies[3].wait()
    own_copy.wait()
    all_near().wait_recv()
    near_ret[...] = expert_rows(chunks - 1)[1].astype(BF16)

    def give_near(p, carry):
        remote(
            near_ret.at[block(p - far_blocks)], near_in.at[block(p - far_blocks)],
            ret_ss.at[1], ret_rs.at[1], "expert", source_at(p),
        ).start()
        return carry

    lax.fori_loop(far_blocks, experts - 1, give_near, 0)
    last_block = blocks(per_chunk - 1, 1)
    own_back = pltpu.make_async_copy(
        near_ret.at[last_block], near_in.at[last_block], local_sem.at[6]
    )
    own_back.start()

    def all_near_back():
        others = blocks(0, near_blocks - 1)
        return remote(
            near_ret.at[others], near_in.at[others], ret_ss.at[1], ret_rs.at[1], "expert", anyone,
        )

    exp_advance(pieces)

    def scatter_copy(refs, c, j, way):
        send, recv, send_sem, recv_sem = refs[1:]
        return remote(
            send.at[way, c, j], recv.at[way, c, j],
            send_sem.at[way, c, j], recv_sem.at[way, c, j], "mp", on_ring(1 - 2 * way),
        )

    def scatter_send(refs, c, j):
        part, send, recv = refs[:3]
        half = send.shape[3]
        for way in (0, 1):
            turn = 1 - 2 * way
            dest = on_ring(turn * (ring // 2 - (j + 1) // 2))
            start = pl.multiple_of(c * 2 * half + ((j + way) % 2) * half, half)
            value = part[dest, pl.ds(start, half), :]
            if j >= 2:
                scatter_copy(refs, c, j - 2, way).wait_recv()
                value = value + recv[way, c, j - 2].astype(F32)
            send[way, c, j] = value.astype(BF16)
            scatter_copy(refs, c, j, way).start()

    def scatter_sum(refs, c, h):
        part, send, recv = refs[:3]
        half = send.shape[3]
        start = pl.multiple_of(c * 2 * half + h * half, half)
        value = part[me, pl.ds(start, half), :]
        for way in (0, 1):
            j = messages - 1 if h == way else messages - 2
            scatter_copy(refs, c, j, way).wait_recv()
            value = value + recv[way, c, j].astype(F32)
        return value

    res_sums = (res_part, rs_send, rs_recv, rs_ss, rs_rs)
    exp_sums = (exp_part, es_send, es_recv, es_ss, es_rs)

    def expert(c):
        rows, part = expert_rows(c)
        for k in range(ring):
            exp_part[k, rows, :] = part[:, k * width : (k + 1) * width]

    def merge():
        own_back.wait()
        all_near_back().wait_recv()
        near_rows = pl.ds(far_rows, chunk_rows)
        for tile in range(tiles):
            rows = pl.ds(tile * res_rows, res_rows)
            back = jnp.dot(table[rows, near_rows], near_in[...], preferred_element_type=F32)
            gates = gate_cols[rows, :]
            for k in range(ring):
                res_part[k, rows, :] += gates * back[:, k * width : (k + 1) * width]

    def give_back(p, carry):
        remote(
            ret_send.at[block(p)], returned.at[block(p)],
            ret_ss.at[0], ret_rs.at[0], "expert", source_at(p),
        ).start()
        return carry

    half_rows = chunk_rows // 2

    def finish(c):
        for h in (0, 1):
            ret_send[pl.ds(c * chunk_rows + h * half_rows, half_rows), :] = scatter_sum(
                exp_sums, c, h
            ).astype(BF16)
        lax.fori_loop(c * per_chunk, (c + 1) * per_chunk, give_back, 0)

    def wave(refs, first, last, *steps):
        def one(c, carry, j=0):
            scatter_send(refs, c, j)
            return carry

        for j in steps:
            if j < messages:
                lax.fori_loop(first, last, functools.partial(one, j=j), 0)

    lead = chunks - 2

    def lead_wave(*steps):
        wave(exp_sums, 0, lead, *steps)

    def last_wave(*steps):
        wave(exp_sums, lead, lead + 1, *steps)

    def res_wave(*steps):
        wave(res_sums, 0, tiles, *steps)

    for c in range(lead):
        expert(c)
        scatter_send(exp_sums, c, 0)
        scatter_send(exp_sums, c, 1)
    all_mid().wait_recv()
    expert(lead)
    last_wave(0, 1)
    lead_wave(2)
    merge()
    res_wave(0)
    last_wave(2)
    lead_wave(3)
    lead_wave(4)
    last_wave(3)
    lead_wave(5)
    res_wave(1)
    lead_wave(6)
    last_wave(4)
    for c in range(lead):
        finish(c)
    last_wave(5)
    res_wave(2)
    last_wave(6)
    res_wave(3)
    finish(lead)
    res_wave(4, 5, 6)

    def all_returned():
        return remote(
            ret_send.at[far], returned.at[far], ret_ss.at[0], ret_rs.at[0], "expert", anyone,
        )

    all_returned().wait_recv()
    half = res_rows // 2
    parts = [pl.ds(at * half, half) for at in range(2 * tiles)]
    gated = [
        gate_cols[rows, :]
        * jnp.dot(table[rows, pl.ds(0, far_rows)], returned[...], preferred_element_type=F32)
        for rows in parts
    ]
    for at, rows in enumerate(parts):
        value = scatter_sum(res_sums, at // 2, at % 2) + gated[at]
        out[rows, :] = value.astype(BF16)

    all_dispatched().wait_send()
    all_near().wait_send()
    all_mid().wait_send()
    all_near_back().wait_send()
    all_returned().wait_send()
    for j in range(gathered):
        for way in (0, 1):
            gather_copy(exp_ring, j, way, False).wait_send()
    for j in range(tok_gathered):
        for way in (0, 1):
            gather_copy(tok_ring, j, way, False).wait_send()

    def drain(refs, c, carry):
        for j in range(messages):
            for way in (0, 1):
                scatter_copy(refs, c, j, way).wait_send()
        return carry

    lax.fori_loop(0, tiles, functools.partial(drain, res_sums), 0)
    lax.fori_loop(0, chunks - 1, functools.partial(drain, exp_sums), 0)


def per_device(
    experts, ring, tokens, gain, w_res_in, w_res_out, w_exp_in, w_exp_out,
    expert_of, slot_of, gate_prob,
):
    count, width = tokens.shape
    model, hidden = w_res_in.shape
    capacity = max(2, 5 * count // (4 * experts))
    slots = -(-capacity // 16) * 16
    chunks = 4 if experts % 8 == 0 else 2
    total = experts * slots
    messages = ring - 1
    near_rows = total // chunks
    far_rows = total - near_rows
    ring_rows = far_rows - (experts // chunks // 4 or 1) * slots

    any_space = pl.BlockSpec(memory_space=pl.ANY)
    sems = pltpu.SemaphoreType.DMA
    tiles = 3 if count % 96 == 0 else 1
    tok_pieces, pieces = 8, 4
    tok_gathered, gathered = messages * tok_pieces // 2, messages * pieces // 2
    res_half, exp_half = count // tiles // 2, total // chunks // 2
    return pl.pallas_call(
        functools.partial(layer_kernel, experts, ring, slots, chunks, tiles, tok_pieces, pieces),
        out_shape=pltpu.VMEM((count, width), BF16),
        in_specs=[any_space] * 9,
        out_specs=pl.BlockSpec(memory_space=pltpu.VMEM),
        scratch_shapes=[
            pltpu.VMEM((count // width, width), jnp.int32),
            pltpu.VMEM((count // width, width), jnp.int32),
            pltpu.VMEM((count // width, width), F32),
            pltpu.VMEM((1, model), F32),
            pltpu.VMEM((ring, count, width), BF16),
            pltpu.VMEM((ring, total, width), BF16),
            pltpu.VMEM((ring_rows, width), BF16),
            pltpu.VMEM((ring, total - ring_rows, width), BF16),
            pltpu.VMEM((model, hidden), BF16),
            pltpu.VMEM((hidden, model), BF16),
            pltpu.VMEM((model, hidden), BF16),
            pltpu.VMEM((hidden, model), BF16),
            pltpu.VMEM((ring, count, width), F32),
            pltpu.VMEM((ring, far_rows, width), F32),
            pltpu.VMEM((2, tiles, messages, res_half, width), BF16),
            pltpu.VMEM((2, tiles, messages, res_half, width), BF16),
            pltpu.VMEM((2, chunks - 1, messages, exp_half, width), BF16),
            pltpu.VMEM((2, chunks - 1, messages, exp_half, width), BF16),
            pltpu.VMEM((far_rows, width), BF16),
            pltpu.VMEM((far_rows, width), BF16),
            pltpu.VMEM((near_rows, model), BF16),
            pltpu.VMEM((near_rows, model), BF16),
            pltpu.VMEM((count, total), BF16),
            pltpu.VMEM((count, width), F32),
            sems((11,)),
            sems((2, tok_gathered)),
            sems((2, tok_gathered)),
            sems((2, gathered)),
            sems((2, gathered)),
            sems((3,)),
            sems((3,)),
            sems((2, tiles, messages)),
            sems((2, tiles, messages)),
            sems((2, chunks - 1, messages)),
            sems((2, chunks - 1, messages)),
            sems((2,)),
            sems((2,)),
        ],
        compiler_params=pltpu.CompilerParams(
            collective_id=0, has_side_effects=True, vmem_limit_bytes=56 * 1024 * 1024
        ),
        name="moe_layer",
    )(
        expert_of.reshape(-1, width), slot_of.reshape(-1, width), gate_prob.reshape(-1, width),
        gain.reshape(1, model), tokens, w_res_in, w_res_out, w_exp_in[0], w_exp_out[0],
    )


def solution(mesh):
    return jax.shard_map(
        functools.partial(per_device, mesh.shape["expert"], mesh.shape["mp"]),
        mesh=mesh,
        in_specs=(
            P(("groups", "expert"), "mp"),
            P(),
            P(None, "mp"),
            P("mp", None),
            P("expert", None, "mp"),
            P("expert", "mp", None),
            P(("groups", "expert")),
            P(("groups", "expert")),
            P(("groups", "expert")),
        ),
        out_specs=P(("groups", "expert"), "mp"),
        check_vma=False,
    )
```
